32 devices in a mesh: dp: 1 (over z), row: 4 (over y), col: 8 (over x, core).
Axes of the slice: x: 4, y: 4, z: 1, core: 2. Of those that a mesh axis runs over, the one named last changes fastest.
The devices are a block of a 4x4x8 slice.
Arguments:
- pair_rep: bfloat16 [1024, 1024, 128], P(('dp', 'row'), 'col')
- res_mask: int32 [1024], P('dp')
- ln_gamma: float32 [128], replicated
- ln_beta: float32 [128], replicated
- w_q: bfloat16 [128, 128], replicated
- w_k: bfloat16 [128, 128], replicated
- w_v: bfloat16 [128, 128], replicated
- w_g: bfloat16 [128, 128], replicated
- w_b: bfloat16 [128, 4], replicated
- w_o: bfloat16 [128, 128], replicated
Outputs:
- output: bfloat16 [1024, 1024, 128], P(('dp', 'row'), 'col')
All inputs are finite; a program needn't handle non-finite values.
Results may differ from the reference program's by a relative error of at most 0.00680541.
Values are sent between devices in bfloat16 or wider.
A program may use at most 768 MiB of HBM per device.

```python
import jax
import jax.numpy as jnp
from jax import lax

NUM_RES = 1024
PAIR_DIM = 128
NUM_HEADS = 4
HEAD_DIM = 32

LN_EPS = 1e-5
MASK_NEG = -1e9


def layer_norm(z_rows, ln_gamma, ln_beta):
    z_float = z_rows.astype(jnp.float32)
    row_mean = jnp.mean(z_float, axis=-1, keepdims=True)
    centered = z_float - row_mean
    row_var = jnp.mean(centered * centered, axis=-1, keepdims=True)
    normed = centered * lax.rsqrt(row_var + LN_EPS) * ln_gamma + ln_beta
    return normed.astype(jnp.bfloat16)


def setup_inputs(seed: int = 0, part: int = 0) -> dict:
    base_key = jax.random.key(seed)
    part_key = jax.random.fold_in(base_key, part)
    key_pair, key_pad = jax.random.split(part_key)
    weight_keys = jax.random.split(base_key, 8)
    width = NUM_HEADS * HEAD_DIM
    pair_rep = jax.random.normal(key_pair, (NUM_RES, NUM_RES, PAIR_DIM), jnp.float32)
    pad_len = jax.random.randint(key_pad, (), NUM_RES // 5, NUM_RES // 2 + 1)
    res_mask = (jnp.arange(NUM_RES) < NUM_RES - pad_len).astype(jnp.int32)
    ln_gamma = 1.0 + 0.3 * jax.random.normal(weight_keys[0], (PAIR_DIM,), jnp.float32)
    ln_beta = NUM_RES ** -0.5 * jax.random.normal(weight_keys[1], (PAIR_DIM,), jnp.float32)
    in_scale = PAIR_DIM ** -0.5
    out_scale = 0.4 * (NUM_RES / width) ** 0.5

    def draw_weight(draw_key, weight_shape, scale_by):
        return (jax.random.normal(draw_key, weight_shape, jnp.float32) * scale_by).astype(jnp.bfloat16)

    return {
        "pair_rep": pair_rep.astype(jnp.bfloat16),
        "res_mask": res_mask,
        "ln_gamma": ln_gamma,
        "ln_beta": ln_beta,
        "w_q": draw_weight(weight_keys[2], (PAIR_DIM, width), in_scale),
        "w_k": draw_weight(weight_keys[3], (PAIR_DIM, width), in_scale),
        "w_v": draw_weight(weight_keys[4], (PAIR_DIM, width), in_scale),
        "w_g": draw_weight(weight_keys[5], (PAIR_DIM, width), in_scale),
        "w_b": draw_weight(weight_keys[6], (PAIR_DIM, NUM_HEADS), in_scale),
        "w_o": draw_weight(weight_keys[7], (width, PAIR_DIM), out_scale),
    }


def reference(pair_rep, res_mask, ln_gamma, ln_beta, w_q, w_k, w_v, w_g, w_b, w_o):
    q_scale = HEAD_DIM ** -0.5
    key_add = jnp.where(res_mask > 0, 0.0, MASK_NEG).astype(jnp.float32)

    def bias_row(z_row):
        normed = layer_norm(z_row, ln_gamma, ln_beta)
        return jnp.dot(normed, w_b, preferred_element_type=jnp.float32).astype(jnp.bfloat16)

    pair_bias = lax.map(bias_row, pair_rep).astype(jnp.float32) + key_add[None, :, None]

    def attend_row(z_row):
        normed = layer_norm(z_row, ln_gamma, ln_beta)

        def heads_of(weight, factor):
            projected = jnp.dot(normed, weight, preferred_element_type=jnp.float32) * factor
            return projected.astype(jnp.bfloat16).astype(jnp.float32).reshape(NUM_RES, NUM_HEADS, HEAD_DIM)

        q_row = heads_of(w_q, q_scale)
        k_row = heads_of(w_k, 1.0)
        v_row = heads_of(w_v, 1.0)
        gate_vals = jax.nn.sigmoid(jnp.dot(normed, w_g, preferred_element_type=jnp.float32))
        logits = jnp.einsum("jhd,khd->jkh", q_row, k_row) + pair_bias
        att_weight = jax.nn.softmax(logits, axis=1)
        attended = jnp.einsum("jkh,khd->jhd", att_weight, v_row).reshape(NUM_RES, NUM_HEADS * HEAD_DIM)
        gated_out = (gate_vals * attended).astype(jnp.bfloat16)
        update = jnp.dot(gated_out, w_o, preferred_element_type=jnp.float32)
        return (z_row.astype(jnp.float32) + update).astype(jnp.bfloat16)

    return lax.map(attend_row, pair_rep)
```

```python
import functools

import jax
import jax.numpy as jnp
from jax import lax
from jax.experimental import pallas as pl
from jax.experimental.pallas import tpu as pltpu
from jax.sharding import PartitionSpec as P

LN_EPS = 1e-5
MASK_NEG = -1e9
J_BLOCK = 256
VMEM_LIMIT = 60 * 1024 * 1024


def normalize(z_rows, ln_gamma, ln_beta):
    z_float = z_rows.astype(jnp.float32)
    row_mean = jnp.mean(z_float, axis=-1, keepdims=True)
    centered = z_float - row_mean
    row_var = jnp.mean(centered * centered, axis=-1, keepdims=True)
    return (centered * lax.rsqrt(row_var + LN_EPS) * ln_gamma + ln_beta).astype(jnp.bfloat16)


def dot_nt(lhs, rhs):
    return lax.dot_general(lhs, rhs, (((1,), (1,)), ((), ())), preferred_element_type=jnp.float32)


def bias_kernel(z_ref, gamma_ref, beta_ref, w_b_ref, out_ref, acc_ref):
    n_heads = out_ref.shape[0]
    rows_step, n_cols, pair_dim = z_ref.shape
    step = pl.program_id(0)
    normed = normalize(z_ref[...].reshape(rows_step * n_cols, pair_dim), gamma_ref[...], beta_ref[...])
    bias = dot_nt(w_b_ref[...], normed)
    for row in range(rows_step):
        for head in range(n_heads):
            acc_ref[head, pl.ds(step * rows_step + row, 1), :] = bias[head : head + 1, row * n_cols : (row + 1) * n_cols]

    @pl.when(step == pl.num_programs(0) - 1)
    def _():
        for head in range(n_heads):
            out_ref[head] = acc_ref[head].T.astype(jnp.bfloat16)


def attend_kernel(z_ref, mask_ref, bias_ref, gamma_ref, beta_ref, w_k_ref, w_qvg_ref, w_o_ref, out_ref, bias_f32, q_scr):
    n_src, _, n_cols, pair_dim = z_ref.shape
    n_heads, n_keys, n_query = bias_ref.shape
    head_dim = pair_dim // n_heads

    @pl.when(pl.program_id(0) == 0)
    def _():
        q_scr[...] = jnp.zeros_like(q_scr)
        for head in range(n_heads):
            for blk in range(0, n_keys, 128):
                key_add = jnp.where(mask_ref[blk : blk + 128, :] > 0, 0.0, MASK_NEG)
                bias_f32[head, blk : blk + 128, :] = bias_ref[head, blk : blk + 128, :].astype(jnp.float32) + key_add

    z_rows = z_ref[...].reshape(n_src * n_cols, pair_dim)
    normed = normalize(z_rows, gamma_ref[...], beta_ref[...])
    k_rows = jnp.dot(normed, w_k_ref[...], preferred_element_type=jnp.float32).astype(jnp.bfloat16)
    qvg = dot_nt(w_qvg_ref[...], normed)
    q_all = (qvg[:pair_dim] * head_dim ** -0.5).astype(jnp.bfloat16)
    v_all = qvg[pair_dim : 2 * pair_dim].astype(jnp.bfloat16)
    gate = jax.nn.sigmoid(qvg[2 * pair_dim :])
    for head in range(n_heads):
        q_scr[head, head * head_dim : (head + 1) * head_dim, :] = q_all[head * head_dim : (head + 1) * head_dim]
    for jb in range(0, n_query, J_BLOCK):
        gated = []
        for head in range(n_heads):
            rows = slice(head * head_dim, (head + 1) * head_dim)
            logits = jnp.dot(k_rows, q_scr[head, :, jb : jb + J_BLOCK], preferred_element_type=jnp.float32)
            logits = logits + bias_f32[head, :, jb : jb + J_BLOCK]
            top = jnp.max(logits, axis=0, keepdims=True)
            weights = jnp.exp(logits - top)
            total = jnp.sum(weights, axis=0, keepdims=True)
            attended = jnp.dot(v_all[rows], weights.astype(jnp.bfloat16), preferred_element_type=jnp.float32)
            gated.append((gate[rows, jb : jb + J_BLOCK] * (attended / total)).astype(jnp.bfloat16))
        u_cols = jnp.concatenate(gated, axis=0)
        update = lax.dot_general(u_cols, w_o_ref[...], (((0,), (0,)), ((), ())), preferred_element_type=jnp.float32)
        result = (z_rows[jb : jb + J_BLOCK].astype(jnp.float32) + update).astype(jnp.bfloat16)
        out_ref[jb // n_cols : (jb + J_BLOCK) // n_cols] = result.reshape(J_BLOCK // n_cols, 1, n_cols, pair_dim)


def solution(mesh):
    n_col_dev = mesh.shape["col"]
    tile_spec = P(("dp", "row"), "col", None)
    replicated = P()
    whole = pl.BlockSpec(memory_space=pltpu.VMEM)

    def local_fn(z_tile, res_mask, ln_gamma, ln_beta, w_q, w_k, w_v, w_g, w_b, w_o):
        n_rows_loc, n_cols, pair_dim = z_tile.shape
        n_heads = w_b.shape[1]
        rows_own = n_rows_loc // n_col_dev
        n_query = res_mask.shape[0]
        gamma, beta = ln_gamma[None, :], ln_beta[None, :]
        w_b_t = jnp.pad(w_b.T, ((0, 8 - n_heads), (0, 0)))
        rows_step = 16
        bias_t = pl.pallas_call(
            bias_kernel,
            grid=(n_rows_loc // rows_step,),
            in_specs=[pl.BlockSpec((rows_step, n_cols, pair_dim), lambda i: (i, 0, 0)), whole, whole, whole],
            out_specs=pl.BlockSpec((n_heads, n_cols, n_rows_loc), lambda i: (0, 0, 0)),
            out_shape=jax.ShapeDtypeStruct((n_heads, n_cols, n_rows_loc), jnp.bfloat16),
            scratch_shapes=[pltpu.VMEM((n_heads, n_rows_loc, n_cols), jnp.float32)],
            compiler_params=pltpu.CompilerParams(vmem_limit_bytes=VMEM_LIMIT),
        )(z_tile, gamma, beta, w_b_t)
        bias_t = lax.all_gather(bias_t, "col", axis=1, tiled=True)
        bias_t = lax.all_gather(bias_t, "row", axis=2, tiled=True)
        z_own = lax.all_to_all(z_tile.reshape(n_col_dev, rows_own, n_cols, pair_dim), "col", 0, 0, tiled=True)
        w_qvg_t = jnp.concatenate([w_q, w_v, w_g], axis=1).T
        blk = pl.BlockSpec((n_col_dev, 1, n_cols, pair_dim), lambda i: (0, i, 0, 0))
        out = pl.pallas_call(
            attend_kernel,
            grid=(rows_own,),
            in_specs=[blk, whole, whole, whole, whole, whole, whole, whole],
            out_specs=blk,
            out_shape=jax.ShapeDtypeStruct(z_own.shape, jnp.bfloat16),
            scratch_shapes=[
                pltpu.VMEM((n_heads, n_query, n_query), jnp.float32),
                pltpu.VMEM((n_heads, pair_dim, n_query), jnp.bfloat16),
            ],
            compiler_params=pltpu.CompilerParams(vmem_limit_bytes=VMEM_LIMIT),
        )(z_own, res_mask[:, None], bias_t, gamma, beta, w_k, w_qvg_t, w_o)
        out = lax.all_to_all(out, "col", 0, 0, tiled=True)
        return out.reshape(n_rows_loc, n_cols, pair_dim)

    return jax.shard_map(
        local_fn,
        mesh=mesh,
        in_specs=(tile_spec, P("dp"), replicated, replicated, replicated, replicated, replicated, replicated, replicated, replicated),
        out_specs=tile_spec,
        check_vma=False,
    )
```

```python
import functools

import jax
import jax.numpy as jnp
from jax import lax
from jax.experimental import pallas as pl
from jax.experimental.pallas import tpu as pltpu
from jax.sharding import PartitionSpec as P

LN_EPS = 1e-5
MASK_NEG = -1e9
J_BLOCK = 256
VMEM_LIMIT = 60 * 1024 * 1024


def normalize(z_rows, ln_gamma, ln_beta):
    z_float = z_rows.astype(jnp.float32)
    row_mean = jnp.mean(z_float, axis=-1, keepdims=True)
    centered = z_float - row_mean
    row_var = jnp.mean(centered * centered, axis=-1, keepdims=True)
    return (centered * lax.rsqrt(row_var + LN_EPS) * ln_gamma + ln_beta).astype(jnp.bfloat16)


def dot_nt(lhs, rhs):
    return lax.dot_general(lhs, rhs, (((1,), (1,)), ((), ())), preferred_element_type=jnp.float32)


def bias_kernel(z_ref, gamma_ref, beta_ref, w_b_ref, out_ref, acc_ref):
    n_heads = out_ref.shape[0]
    rows_step, n_cols, pair_dim = z_ref.shape
    step = pl.program_id(0)
    normed = normalize(z_ref[...].reshape(rows_step * n_cols, pair_dim), gamma_ref[...], beta_ref[...])
    bias = dot_nt(w_b_ref[...], normed)
    for row in range(rows_step):
        for head in range(n_heads):
            acc_ref[head, pl.ds(step * rows_step + row, 1), :] = bias[head : head + 1, row * n_cols : (row + 1) * n_cols]

    @pl.when(step == pl.num_programs(0) - 1)
    def _():
        for head in range(n_heads):
            out_ref[head] = acc_ref[head].T.astype(jnp.bfloat16)


def attend_kernel(z_ref, mask_ref, bias_ref, gamma_ref, beta_ref, w_k_ref, w_qvg_ref, w_o_ref, out_ref, bias_f32, q_scr, gate_scr):
    n_src, _, n_cols, pair_dim = z_ref.shape
    n_heads, n_keys, n_query = bias_ref.shape
    head_dim = pair_dim // n_heads

    @pl.when(pl.program_id(0) == 0)
    def _():
        q_scr[...] = jnp.zeros_like(q_scr)
        for head in range(n_heads):
            for blk in range(0, n_keys, 128):
                key_add = jnp.where(mask_ref[blk : blk + 128, :] > 0, 0.0, MASK_NEG)
                bias_f32[head, blk : blk + 128, :] = bias_ref[head, blk : blk + 128, :].astype(jnp.float32) + key_add

    z_rows = z_ref[...].reshape(n_src * n_cols, pair_dim)
    normed = normalize(z_rows, gamma_ref[...], beta_ref[...])
    k_rows = jnp.dot(normed, w_k_ref[...], preferred_element_type=jnp.float32).astype(jnp.bfloat16)
    qvg = dot_nt(w_qvg_ref[...], normed)
    q_all = (qvg[:pair_dim] * head_dim ** -0.5).astype(jnp.bfloat16)
    v_all = qvg[pair_dim : 2 * pair_dim].astype(jnp.bfloat16)
    for head in range(n_heads):
        q_scr[head, head * head_dim : (head + 1) * head_dim, :] = q_all[head * head_dim : (head + 1) * head_dim]
    gate_scr[...] = jax.nn.sigmoid(qvg[2 * pair_dim :])

    def one_block(blk_idx, _):
        jb = pl.multiple_of(blk_idx * J_BLOCK, J_BLOCK)
        gated = []
        for head in range(n_heads):
            rows = slice(head * head_dim, (head + 1) * head_dim)
            logits = jnp.dot(k_rows, q_scr[head, :, pl.ds(jb, J_BLOCK)], preferred_element_type=jnp.float32)
            logits = logits + bias_f32[head, :, pl.ds(jb, J_BLOCK)]
            top = jnp.max(logits, axis=0, keepdims=True)
            weights = jnp.exp(logits - top)
            total = jnp.sum(weights, axis=0, keepdims=True)
            attended = jnp.dot(v_all[rows], weights.astype(jnp.bfloat16), preferred_element_type=jnp.float32)
            gated.append((gate_scr[rows, pl.ds(jb, J_BLOCK)] * (attended / total)).astype(jnp.bfloat16))
        u_cols = jnp.concatenate(gated, axis=0)
        update = lax.dot_general(u_cols, w_o_ref[...], (((0,), (0,)), ((), ())), preferred_element_type=jnp.float32)
        n_blk = J_BLOCK // n_cols
        z_blk = z_ref[pl.ds(blk_idx * n_blk, n_blk)].reshape(J_BLOCK, pair_dim).astype(jnp.float32)
        out_ref[pl.ds(blk_idx * n_blk, n_blk)] = (z_blk + update).astype(jnp.bfloat16).reshape(n_blk, 1, n_cols, pair_dim)
        return 0

    lax.fori_loop(0, n_query // J_BLOCK, one_block, 0)


MESH = pl.DeviceIdType.MESH
LOG2E = 1.4426950408889634
STEP_ROWS = 4
KEY_CHUNK = 416


def fold8(values, op):
    return op(values.reshape(values.shape[0] // 8, 8, values.shape[1]), axis=0)


def fused_kernel(
    n_dev, n_row_dev, n_heads, n_used,
    z_hbm, mask_ref, gamma_ref, beta_ref, w_b_ref, w_k_ref, w_qvg_ref, w_o_ref, eye_ref,
    out_hbm,
    z_in, b_acc, b_all, z_rows, a_scr, k_scr, q_scr, v_scr, g_scr, s_scr, u_scr, o_scr,
    in_sem, own_sem, z_send, z_recv, bx_send, bx_recv, by_send, by_recv, bd_send, bd_recv, o_send, o_recv, o_own,
):
    me, row = lax.axis_index("col"), lax.axis_index("row")
    n_rows_loc, n_cols, pair_dim = z_hbm.shape
    head_dim = pair_dim // n_heads
    rows_own = n_rows_loc // n_dev
    n_steps = rows_own // STEP_ROWS
    n_chip = n_dev // 2
    blk_rows = n_rows_loc // n_cols
    chunk = z_in.shape[1]
    n_chunks = n_rows_loc // chunk
    col_at = lambda d: lax.rem(me + d + n_dev, n_dev)
    row_at = lambda d: lax.rem(row + d + n_row_dev, n_row_dev)
    partner = me + 1 - 2 * lax.rem(me, 2)

    barrier = pltpu.get_barrier_semaphore()
    for d in range(1, n_dev):
        pl.semaphore_signal(barrier, inc=1, device_id={"col": col_at(d)}, device_id_type=MESH)
    for d in range(1, n_row_dev):
        pl.semaphore_signal(barrier, inc=1, device_id={"row": row_at(d)}, device_id_type=MESH)
    pl.semaphore_wait(barrier, n_dev + n_row_dev - 2)

    def z_copy(step, d, to, at):
        return pltpu.make_async_remote_copy(
            z_hbm.at[pl.ds(to * rows_own + step * STEP_ROWS, STEP_ROWS)], z_rows.at[at, pl.ds(step * STEP_ROWS, STEP_ROWS)],
            z_send.at[step, d], z_recv.at[step, d], device_id={"col": to}, device_id_type=MESH)

    def start_z(step):
        for d in range(1, n_dev):
            z_copy(step, d, col_at(d), me).start()

    def b_tile(src_row, src_col):
        return b_all.at[pl.ds(src_row * blk_rows, blk_rows), :, pl.ds(pl.multiple_of(src_col * n_cols, n_cols), n_cols), :]

    def b_copy(src_row, src_col, send, recv, target):
        tile = b_tile(src_row, src_col)
        return pltpu.make_async_remote_copy(tile, tile, send, recv, device_id=target, device_id_type=MESH)

    def bx(d, src_col):
        return b_copy(row, src_col, bx_send.at[d], bx_recv.at[d], {"col": col_at(2 * d)})

    def by(t, e, src_row):
        return b_copy(src_row, col_at(-2 * t), by_send.at[t, e], by_recv.at[t, e], {"row": row_at(e)})

    def bd(t, e, base):
        return b_copy(row_at(-e), lax.rem(base - 2 * t + n_dev, n_dev), bd_send.at[t, e], bd_recv.at[t, e], {"col": partner})

    def out_copy(step, d, to, at):
        return pltpu.make_async_remote_copy(
            o_scr.at[lax.rem(step, 2), to], out_hbm.at[pl.ds(at * rows_own + step * STEP_ROWS, STEP_ROWS)],
            o_send.at[lax.rem(step, 2), d], o_recv.at[step, d], device_id={"col": to}, device_id_type=MESH)

    def out_own(step):
        return pltpu.make_async_copy(
            o_scr.at[lax.rem(step, 2), me], out_hbm.at[pl.ds(me * rows_own + step * STEP_ROWS, STEP_ROWS)], o_own.at[lax.rem(step, 2)])

    own_rows = pltpu.make_async_copy(z_hbm.at[pl.ds(me * rows_own, rows_own)], z_rows.at[me], own_sem)
    own_rows.start()
    start_z(0)
    start_z(1)

    def load_chunk(idx):
        return pltpu.make_async_copy(z_hbm.at[pl.ds(idx * chunk, chunk)], z_in.at[lax.rem(idx, 2)], in_sem.at[lax.rem(idx, 2)])

    load_chunk(0).start()

    def bias_chunk(idx, _):
        @pl.when(idx + 1 < n_chunks)
        def _():
            load_chunk(idx + 1).start()

        load_chunk(idx).wait()
        normed = normalize(z_in[lax.rem(idx, 2)].reshape(chunk * n_cols, pair_dim), gamma_ref[...], beta_ref[...])
        bias = dot_nt(w_b_ref[...], normed)
        for r in range(chunk):
            for head in range(n_heads):
                b_acc[head, pl.ds(idx * chunk + r, 1), :] = bias[head : head + 1, r * n_cols : (r + 1) * n_cols]
        return 0

    lax.fori_loop(0, n_chunks, bias_chunk, 0)
    own_cols = pl.ds(pl.multiple_of(me * n_cols, n_cols), n_cols)
    for blk in range(blk_rows):
        for head in range(n_heads):
            tile = b_acc[head, blk * n_cols : (blk + 1) * n_cols, :].T
            b_all[row * blk_rows + blk, head, own_cols, :] = jnp.where(mask_ref[...] > 0, tile, MASK_NEG).astype(jnp.bfloat16)

    def clear(idx, _):
        q_scr[idx] = jnp.zeros(q_scr.shape[1:], q_scr.dtype)
        return 0

    lax.fori_loop(0, q_scr.shape[0], clear, 0)

    for d in range(1, n_chip):
        bx(d, me).start()
    for e in range(1, n_row_dev):
        by(0, e, row).start()
    bd(0, 0, me).start()
    for step in range(2, n_steps):
        start_z(step)
    for t in range(1, n_chip):
        bx(t, col_at(-2 * t)).wait_recv()
        for e in range(1, n_row_dev):
            by(t, e, row).start()
        bd(t, 0, me).start()

    def prologue(step):
        for d in range(1, n_dev):
            z_copy(step, d, me, col_at(-d)).wait_recv()
        for r in range(STEP_ROWS):
            normed = normalize(z_rows[:, step * STEP_ROWS + r].reshape(n_dev * n_cols, pair_dim), gamma_ref[...], beta_ref[...])
            a_scr[r] = normed
            qvg = dot_nt(w_qvg_ref[...], normed)
            pair, half = r // 2, r % 2
            q_all = (qvg[:pair_dim] * head_dim ** -0.5).astype(jnp.bfloat16)
            v_all = qvg[pair_dim : 2 * pair_dim].astype(jnp.bfloat16)
            gate = jax.nn.sigmoid(qvg[2 * pair_dim :])
            for head in range(n_heads):
                hs = slice(head * head_dim, (head + 1) * head_dim)
                v_scr[pair, head, half * head_dim : (half + 1) * head_dim, :] = v_all[hs]
                for jb in range(n_dev):
                    js = slice(jb * n_cols, (jb + 1) * n_cols)
                    ls = slice(half * n_cols, (half + 1) * n_cols)
                    q_scr[jb * 2 + pair, head, r * head_dim : (r + 1) * head_dim, ls] = q_all[hs, js]
                    g_scr[jb * 2 + pair, head, :, ls] = gate[hs, js]
        for k0 in range(0, n_used, 128):
            kn = min(128, n_used - k0)
            a_cat = jnp.concatenate([a_scr[r, k0 : k0 + kn, :] for r in range(STEP_ROWS)], axis=1)
            k_all = jnp.dot(a_cat, w_k_ref[...], preferred_element_type=jnp.float32).astype(jnp.bfloat16)
            for head in range(n_heads):
                k_scr[head, k0 : k0 + kn, :] = k_all[:, head * pair_dim : (head + 1) * pair_dim]

    key_blocks = [(k0, min(KEY_CHUNK, n_used - k0)) for k0 in range(0, n_used, KEY_CHUNK)]
    n_units = n_dev * 2

    def logits_of(head, unit, slot, k0, kn, top):
        lhs = jnp.concatenate([k_scr[head, k0 : k0 + kn, :], b_all[lax.div(unit, 2), head, k0 : k0 + kn, :]], axis=1)
        rhs = jnp.concatenate([q_scr[unit, head], eye_ref[...]], axis=0)
        scaled = jnp.dot(lhs, rhs, preferred_element_type=jnp.float32) * LOG2E
        s_scr[slot, k0 : k0 + kn, :] = scaled
        new_top = fold8(scaled, jnp.max)
        return new_top if top is None else jnp.maximum(top, new_top)

    def update_unit(step, unit):
        jb, pair = lax.div(unit, 2), lax.rem(unit, 2)
        update = lax.dot_general(u_scr[pair], w_o_ref[...], (((0,), (0,)), ((), ())), preferred_element_type=jnp.float32)
        for half in range(2):
            r = pair * 2 + half
            z_blk = z_rows[jb, step * STEP_ROWS + r].astype(jnp.float32)
            o_scr[lax.rem(step, 2), jb, r] = (z_blk + update[half * n_cols : (half + 1) * n_cols]).astype(jnp.bfloat16)

    def attend(step):
        def one_unit(unit, top):
            pair = lax.rem(unit, 2)
            unit_next = jnp.minimum(unit + 1, n_units - 1)
            for head in range(n_heads):
                head_next, from_unit = (head + 1, unit) if head + 1 < n_heads else (0, unit_next)
                top_row = jnp.max(top, axis=0, keepdims=True)
                top_next = total = attended = None
                for k0, kn in key_blocks:
                    top_next = logits_of(head_next, from_unit, (head + 1) % 2, k0, kn, top_next)
                    weights = jnp.exp2(s_scr[head % 2, k0 : k0 + kn, :] - top_row)
                    part = fold8(weights, jnp.sum)
                    total = part if total is None else total + part
                    prod = jnp.dot(v_scr[pair, head, :, k0 : k0 + kn], weights.astype(jnp.bfloat16), preferred_element_type=jnp.float32)
                    attended = prod if attended is None else attended + prod
                inv = 1.0 / jnp.sum(total, axis=0, keepdims=True)
                picked = jnp.concatenate([attended[:head_dim, :n_cols], attended[head_dim:, n_cols:]], axis=1)
                u_scr[pair, head * head_dim : (head + 1) * head_dim, :] = (g_scr[unit, head] * (picked * inv)).astype(jnp.bfloat16)
                top = top_next
                if head == 0:
                    update_unit(step, jnp.maximum(unit - 1, 0))
            return top

        top = None
        for k0, kn in key_blocks:
            top = logits_of(0, 0, 0, k0, kn, top)
        lax.fori_loop(0, n_units, one_unit, top)
        update_unit(step, n_units - 1)

    own_rows.wait()
    prologue(0)
    for t in range(n_chip):
        for e in range(1, n_row_dev):
            by(t, e, row_at(-e)).wait_recv()
            bd(t, e, me).start()
    for t in range(n_chip):
        for e in range(n_row_dev):
            bd(t, e, partner).wait_recv()

    def one_step(step, _):
        @pl.when(step >= 2)
        def _():
            for d in range(1, n_dev):
                out_copy(step - 2, d, col_at(d), me).wait_send()
            out_own(step - 2).wait()

        @pl.when(step >= 1)
        def _():
            prologue(step)

        attend(step)
        for d in range(1, n_dev):
            out_copy(step, d, col_at(d), me).start()
        out_own(step).start()
        return 0

    lax.fori_loop(0, n_steps, one_step, 0)

    for step in range(n_steps - 2, n_steps):
        for d in range(1, n_dev):
            out_copy(step, d, col_at(d), me).wait_send()
        out_own(step).wait()
    for d in range(1, n_chip):
        bx(d, me).wait_send()
    for t in range(n_chip):
        for e in range(1, n_row_dev):
            by(t, e, row).wait_send()
        for e in range(n_row_dev):
            bd(t, e, me).wait_send()

    def drain(step, _):
        for d in range(1, n_dev):
            z_copy(step, d, col_at(d), me).wait_send()
            out_copy(step, d, me, col_at(-d)).wait_recv()
        return 0

    lax.fori_loop(0, n_steps, drain, 0)


def fused_path(mesh, z_tile, res_mask, ln_gamma, ln_beta, w_q, w_k, w_v, w_g, w_b, w_o):
    n_dev, n_row_dev = mesh.shape["col"], mesh.shape["row"]
    n_rows_loc, n_cols, pair_dim = z_tile.shape
    n_heads = w_b.shape[1]
    n_query = res_mask.shape[0]
    n_used = -(-(n_query - n_query // 5) // 64) * 64
    rows_own = n_rows_loc // n_dev
    n_steps = rows_own // STEP_ROWS
    head_dim = pair_dim // n_heads
    mask_own = lax.dynamic_slice_in_dim(res_mask, lax.axis_index("col") * n_cols, n_cols)[:, None]
    w_b_t = jnp.pad(w_b.T, ((0, 8 - n_heads), (0, 0)))
    w_qvg_t = jnp.concatenate([w_q, w_v, w_g], axis=1).T
    spread = jnp.eye(STEP_ROWS, dtype=w_k.dtype)
    w_k_wide = jnp.einsum("rs,chd->rchsd", spread, w_k.reshape(pair_dim, n_heads, head_dim)).reshape(STEP_ROWS * pair_dim, n_heads * pair_dim)
    eye = jnp.tile(jnp.eye(n_cols, dtype=jnp.bfloat16), (1, 2))
    whole = pl.BlockSpec(memory_space=pltpu.VMEM)
    hbm = pl.BlockSpec(memory_space=pl.ANY)
    bf16, f32, dma = jnp.bfloat16, jnp.float32, pltpu.SemaphoreType.DMA
    n_units = n_dev * 2
    return pl.pallas_call(
        functools.partial(fused_kernel, n_dev, n_row_dev, n_heads, n_used),
        in_specs=[hbm] + [whole] * 8,
        out_specs=hbm,
        out_shape=jax.ShapeDtypeStruct(z_tile.shape, bf16),
        scratch_shapes=[
            pltpu.VMEM((2, 16, n_cols, pair_dim), bf16),
            pltpu.VMEM((n_heads, n_rows_loc, n_cols), f32),
            pltpu.VMEM((n_query // n_cols, n_heads, n_query, n_cols), bf16),
            pltpu.VMEM((n_dev, rows_own, n_cols, pair_dim), bf16),
            pltpu.VMEM((STEP_ROWS, n_query, pair_dim), bf16),
            pltpu.VMEM((n_heads, n_query, STEP_ROWS * head_dim), bf16),
            pltpu.VMEM((n_units, n_heads, STEP_ROWS * head_dim, 2 * n_cols), bf16),
            pltpu.VMEM((2, n_heads, 2 * head_dim, n_query), bf16),
            pltpu.VMEM((n_units, n_heads, head_dim, 2 * n_cols), f32),
            pltpu.VMEM((2, n_used, 2 * n_cols), f32),
            pltpu.VMEM((2, pair_dim, 2 * n_cols), bf16),
            pltpu.VMEM((2, n_dev, STEP_ROWS, n_cols, pair_dim), bf16),
            dma((2,)), dma, dma((n_steps, n_dev)), dma((n_steps, n_dev)),
            dma((n_dev // 2,)), dma((n_dev // 2,)), dma((n_dev // 2, n_row_dev)), dma((n_dev // 2, n_row_dev)),
            dma((n_dev // 2, n_row_dev)), dma((n_dev // 2, n_row_dev)), dma((2, n_dev)), dma((n_steps, n_dev)), dma((2,)),
        ],
        compiler_params=pltpu.CompilerParams(collective_id=0, has_side_effects=True, vmem_limit_bytes=VMEM_LIMIT),
    )(z_tile, mask_own, ln_gamma[None, :], ln_beta[None, :], w_b_t, w_k_wide, w_qvg_t, w_o, eye)


def solution(mesh):
    n_col_dev = mesh.shape["col"]
    tile_spec = P(("dp", "row"), "col", None)
    replicated = P()
    whole = pl.BlockSpec(memory_space=pltpu.VMEM)

    def whole_keys_path(z_tile, res_mask, ln_gamma, ln_beta, w_q, w_k, w_v, w_g, w_b, w_o):
        n_rows_loc, n_cols, pair_dim = z_tile.shape
        n_heads = w_b.shape[1]
        rows_own = n_rows_loc // n_col_dev
        n_query = res_mask.shape[0]
        gamma, beta = ln_gamma[None, :], ln_beta[None, :]
        w_b_t = jnp.pad(w_b.T, ((0, 8 - n_heads), (0, 0)))
        rows_step = 16
        bias_t = pl.pallas_call(
            bias_kernel,
            grid=(n_rows_loc // rows_step,),
            in_specs=[pl.BlockSpec((rows_step, n_cols, pair_dim), lambda i: (i, 0, 0)), whole, whole, whole],
            out_specs=pl.BlockSpec((n_heads, n_cols, n_rows_loc), lambda i: (0, 0, 0)),
            out_shape=jax.ShapeDtypeStruct((n_heads, n_cols, n_rows_loc), jnp.bfloat16),
            scratch_shapes=[pltpu.VMEM((n_heads, n_rows_loc, n_cols), jnp.float32)],
            compiler_params=pltpu.CompilerParams(vmem_limit_bytes=VMEM_LIMIT),
        )(z_tile, gamma, beta, w_b_t)
        bias_t = lax.all_gather(bias_t, "col", axis=1, tiled=True)
        bias_t = lax.all_gather(bias_t, "row", axis=2, tiled=True)
        z_own = lax.all_to_all(z_tile.reshape(n_col_dev, rows_own, n_cols, pair_dim), "col", 0, 0, tiled=True)
        w_qvg_t = jnp.concatenate([w_q, w_v, w_g], axis=1).T
        blk = pl.BlockSpec((n_col_dev, 1, n_cols, pair_dim), lambda i: (0, i, 0, 0))
        out = pl.pallas_call(
            attend_kernel,
            grid=(rows_own,),
            in_specs=[blk, whole, whole, whole, whole, whole, whole, whole],
            out_specs=blk,
            out_shape=jax.ShapeDtypeStruct(z_own.shape, jnp.bfloat16),
            scratch_shapes=[
                pltpu.VMEM((n_heads, n_query, n_query), jnp.float32),
                pltpu.VMEM((n_heads, pair_dim, n_query), jnp.bfloat16),
                pltpu.VMEM((pair_dim, n_query), jnp.float32),
            ],
            compiler_params=pltpu.CompilerParams(vmem_limit_bytes=VMEM_LIMIT),
        )(z_own, res_mask[:, None], bias_t, gamma, beta, w_k, w_qvg_t, w_o)
        out = lax.all_to_all(out, "col", 0, 0, tiled=True)
        return out.reshape(n_rows_loc, n_cols, pair_dim)

    def local_fn(*args):
        _, _, ln_gamma, ln_beta, w_q, w_k, _, _, w_b, _ = args
        pair_dim, n_heads = w_b.shape
        largest = (pair_dim ** 0.5 * jnp.abs(ln_gamma) + jnp.abs(ln_beta))[:, None]
        bound = lambda weight: jnp.sum(largest * jnp.abs(weight.astype(jnp.float32)), axis=0)
        logit_bound = jnp.sum(bound(w_q) * bound(w_k)) + jnp.max(bound(w_b))
        return lax.cond(logit_bound < 1e8, functools.partial(fused_path, mesh), whole_keys_path, *args)

    return jax.shard_map(
        local_fn,
        mesh=mesh,
        in_specs=(tile_spec, P("dp"), replicated, replicated, replicated, replicated, replicated, replicated, replicated, replicated),
        out_specs=tile_spec,
        check_vma=False,
    )
```

```python
import functools

import jax
import jax.numpy as jnp
from jax import lax
from jax.experimental import pallas as pl
from jax.experimental.pallas import tpu as pltpu
from jax.sharding import PartitionSpec as P

LN_EPS = 1e-5
MASK_NEG = -1e9
J_BLOCK = 256
VMEM_LIMIT = 60 * 1024 * 1024


def normalize(z_rows, ln_gamma, ln_beta):
    z_float = z_rows.astype(jnp.float32)
    row_mean = jnp.mean(z_float, axis=-1, keepdims=True)
    centered = z_float - row_mean
    row_var = jnp.mean(centered * centered, axis=-1, keepdims=True)
    return (centered * lax.rsqrt(row_var + LN_EPS) * ln_gamma + ln_beta).astype(jnp.bfloat16)


def dot_nt(lhs, rhs):
    return lax.dot_general(lhs, rhs, (((1,), (1,)), ((), ())), preferred_element_type=jnp.float32)


def bias_kernel(z_ref, gamma_ref, beta_ref, w_b_ref, out_ref, acc_ref):
    n_heads = out_ref.shape[0]
    rows_step, n_cols, pair_dim = z_ref.shape
    step = pl.program_id(0)
    normed = normalize(z_ref[...].reshape(rows_step * n_cols, pair_dim), gamma_ref[...], beta_ref[...])
    bias = dot_nt(w_b_ref[...], normed)
    for row in range(rows_step):
        for head in range(n_heads):
            acc_ref[head, pl.ds(step * rows_step + row, 1), :] = bias[head : head + 1, row * n_cols : (row + 1) * n_cols]

    @pl.when(step == pl.num_programs(0) - 1)
    def _():
        for head in range(n_heads):
            out_ref[head] = acc_ref[head].T.astype(jnp.bfloat16)


def attend_kernel(z_ref, mask_ref, bias_ref, gamma_ref, beta_ref, w_k_ref, w_qvg_ref, out_ref, bias_f32, q_scr, gate_scr):
    n_src, _, n_cols, pair_dim = z_ref.shape
    n_heads, n_keys, n_query = bias_ref.shape
    head_dim = pair_dim // n_heads

    @pl.when(pl.program_id(0) == 0)
    def _():
        q_scr[...] = jnp.zeros_like(q_scr)
        for head in range(n_heads):
            for blk in range(0, n_keys, 128):
                key_add = jnp.where(mask_ref[blk : blk + 128, :] > 0, 0.0, MASK_NEG)
                bias_f32[head, blk : blk + 128, :] = bias_ref[head, blk : blk + 128, :].astype(jnp.float32) + key_add

    z_rows = z_ref[...].reshape(n_src * n_cols, pair_dim)
    normed = normalize(z_rows, gamma_ref[...], beta_ref[...])
    k_rows = jnp.dot(normed, w_k_ref[...], preferred_element_type=jnp.float32).astype(jnp.bfloat16)
    qvg = dot_nt(w_qvg_ref[...], normed)
    q_all = (qvg[:pair_dim] * head_dim ** -0.5).astype(jnp.bfloat16)
    v_all = qvg[pair_dim : 2 * pair_dim].astype(jnp.bfloat16)
    for head in range(n_heads):
        q_scr[head, head * head_dim : (head + 1) * head_dim, :] = q_all[head * head_dim : (head + 1) * head_dim]
    gate_scr[...] = jax.nn.sigmoid(qvg[2 * pair_dim :])

    def one_block(blk_idx, _):
        jb = pl.multiple_of(blk_idx * J_BLOCK, J_BLOCK)
        gated = []
        for head in range(n_heads):
            rows = slice(head * head_dim, (head + 1) * head_dim)
            logits = jnp.dot(k_rows, q_scr[head, :, pl.ds(jb, J_BLOCK)], preferred_element_type=jnp.float32)
            logits = logits + bias_f32[head, :, pl.ds(jb, J_BLOCK)]
            top = jnp.max(logits, axis=0, keepdims=True)
            weights = jnp.exp(logits - top)
            total = jnp.sum(weights, axis=0, keepdims=True)
            attended = jnp.dot(v_all[rows], weights.astype(jnp.bfloat16), preferred_element_type=jnp.float32)
            gated.append((gate_scr[rows, pl.ds(jb, J_BLOCK)] * (attended / total)).astype(jnp.bfloat16))
        u_cols = jnp.concatenate(gated, axis=0)
        for part in range(J_BLOCK // n_cols):
            out_ref[blk_idx * (J_BLOCK // n_cols) + part, 0] = u_cols[:, part * n_cols : (part + 1) * n_cols]
        return 0

    lax.fori_loop(0, n_query // J_BLOCK, one_block, 0)


MESH = pl.DeviceIdType.MESH
LOG2E = 1.4426950408889634
STEP_ROWS = 4
KEY_CHUNK = 416


def fold8(values, op):
    return op(values.reshape(values.shape[0] // 8, 8, values.shape[1]), axis=0)


def fused_kernel(
    n_dev, n_row_dev, n_heads, n_used,
    z_hbm, mask_ref, gamma_ref, beta_ref, w_b_ref, w_k_ref, w_qvg_ref, eye_ref,
    out_hbm,
    z_in, b_acc, b_all, z_rows, a_scr, k_scr, q_scr, v_scr, g_scr, s_scr, o_scr,
    in_sem, own_sem, z_send, z_recv, bx_send, bx_recv, by_send, by_recv, bd_send, bd_recv, o_send, o_recv, o_own,
):
    me, row = lax.axis_index("col"), lax.axis_index("row")
    n_rows_loc, n_cols, pair_dim = z_hbm.shape
    head_dim = pair_dim // n_heads
    rows_own = n_rows_loc // n_dev
    n_steps = rows_own // STEP_ROWS
    n_chip = n_dev // 2
    blk_rows = n_rows_loc // n_cols
    chunk = z_in.shape[1]
    n_chunks = n_rows_loc // chunk
    col_at = lambda d: lax.rem(me + d + n_dev, n_dev)
    row_at = lambda d: lax.rem(row + d + n_row_dev, n_row_dev)
    partner = me + 1 - 2 * lax.rem(me, 2)

    barrier = pltpu.get_barrier_semaphore()
    for d in range(1, n_dev):
        pl.semaphore_signal(barrier, inc=1, device_id={"col": col_at(d)}, device_id_type=MESH)
    for d in range(1, n_row_dev):
        pl.semaphore_signal(barrier, inc=1, device_id={"row": row_at(d)}, device_id_type=MESH)
    pl.semaphore_wait(barrier, n_dev + n_row_dev - 2)

    def z_copy(step, d, to, at):
        return pltpu.make_async_remote_copy(
            z_hbm.at[pl.ds(to * rows_own + step * STEP_ROWS, STEP_ROWS)], z_rows.at[at, pl.ds(step * STEP_ROWS, STEP_ROWS)],
            z_send.at[step, d], z_recv.at[step, d], device_id={"col": to}, device_id_type=MESH)

    def start_z(step):
        for d in range(1, n_dev):
            z_copy(step, d, col_at(d), me).start()

    def b_tile(src_row, src_col):
        return b_all.at[pl.ds(src_row * blk_rows, blk_rows), :, pl.ds(pl.multiple_of(src_col * n_cols, n_cols), n_cols), :]

    def b_copy(src_row, src_col, send, recv, target):
        tile = b_tile(src_row, src_col)
        return pltpu.make_async_remote_copy(tile, tile, send, recv, device_id=target, device_id_type=MESH)

    def bx(d, src_col):
        return b_copy(row, src_col, bx_send.at[d], bx_recv.at[d], {"col": col_at(2 * d)})

    def by(t, e, src_row):
        return b_copy(src_row, col_at(-2 * t), by_send.at[t, e], by_recv.at[t, e], {"row": row_at(e)})

    def bd(t, e, base):
        return b_copy(row_at(-e), lax.rem(base - 2 * t + n_dev, n_dev), bd_send.at[t, e], bd_recv.at[t, e], {"col": partner})

    def out_copy(step, d, to, at):
        return pltpu.make_async_remote_copy(
            o_scr.at[lax.rem(step, 2), to], out_hbm.at[pl.ds(at * rows_own + step * STEP_ROWS, STEP_ROWS)],
            o_send.at[lax.rem(step, 2), d], o_recv.at[step, d], device_id={"col": to}, device_id_type=MESH)

    def out_own(step):
        return pltpu.make_async_copy(
            o_scr.at[lax.rem(step, 2), me], out_hbm.at[pl.ds(me * rows_own + step * STEP_ROWS, STEP_ROWS)], o_own.at[lax.rem(step, 2)])

    own_rows = pltpu.make_async_copy(z_hbm.at[pl.ds(me * rows_own, rows_own)], z_rows.at[me], own_sem)
    own_rows.start()
    start_z(0)

    def load_chunk(idx):
        return pltpu.make_async_copy(z_hbm.at[pl.ds(idx * chunk, chunk)], z_in.at[lax.rem(idx, 2)], in_sem.at[lax.rem(idx, 2)])

    load_chunk(0).start()

    def bias_chunk(idx, _):
        @pl.when(idx + 1 < n_chunks)
        def _():
            load_chunk(idx + 1).start()

        load_chunk(idx).wait()
        normed = normalize(z_in[lax.rem(idx, 2)].reshape(chunk * n_cols, pair_dim), gamma_ref[...], beta_ref[...])
        bias = dot_nt(w_b_ref[...], normed)
        for r in range(chunk):
            for head in range(n_heads):
                b_acc[head, pl.ds(idx * chunk + r, 1), :] = bias[head : head + 1, r * n_cols : (r + 1) * n_cols]
        return 0

    lax.fori_loop(0, n_chunks, bias_chunk, 0)
    own_cols = pl.ds(pl.multiple_of(me * n_cols, n_cols), n_cols)
    for blk in range(blk_rows):
        for head in range(n_heads):
            tile = jnp.where(mask_ref[pl.ds(me, 1), :] > 0, b_acc[head, blk * n_cols : (blk + 1) * n_cols, :], MASK_NEG)
            b_all[row * blk_rows + blk, head, own_cols, :] = tile.T.astype(jnp.bfloat16)

    def clear(idx, _):
        q_scr[idx] = jnp.zeros(q_scr.shape[1:], q_scr.dtype)
        return 0

    lax.fori_loop(0, q_scr.shape[0], clear, 0)

    for d in range(1, n_chip):
        bx(d, me).start()
    for e in range(1, n_row_dev):
        by(0, e, row).start()
    bd(0, 0, me).start()
    for step in range(1, n_steps):
        start_z(step)
    for t in range(1, n_chip):
        bx(t, col_at(-2 * t)).wait_recv()
        for e in range(1, n_row_dev):
            by(t, e, row).start()
        bd(t, 0, me).start()

    def wait_z(step):
        for d in range(1, n_dev):
            z_copy(step, d, me, col_at(-d)).wait_recv()

    def prologue(step):
        for r in range(STEP_ROWS):
            normed = normalize(z_rows[:, step * STEP_ROWS + r].reshape(n_dev * n_cols, pair_dim), gamma_ref[...], beta_ref[...])
            a_scr[r] = normed
            qvg = dot_nt(w_qvg_ref[...], normed)
            pair, half = r // 2, r % 2
            q_all = (qvg[:pair_dim] * head_dim ** -0.5).astype(jnp.bfloat16)
            v_all = qvg[pair_dim : 2 * pair_dim].astype(jnp.bfloat16)
            gate = jax.nn.sigmoid(qvg[2 * pair_dim :])
            for head in range(n_heads):
                hs = slice(head * head_dim, (head + 1) * head_dim)
                v_scr[pair, head, half * head_dim : (half + 1) * head_dim, :] = v_all[hs]
                for jb in range(n_dev):
                    js = slice(jb * n_cols, (jb + 1) * n_cols)
                    ls = slice(half * n_cols, (half + 1) * n_cols)
                    q_scr[jb * 2 + pair, head, r * head_dim : (r + 1) * head_dim, ls] = q_all[hs, js]
                    g_scr[jb * 2 + pair, head, :, ls] = gate[hs, js]
        for k0 in range(0, n_used, 128):
            kn = min(128, n_used - k0)
            a_cat = jnp.concatenate([a_scr[r, k0 : k0 + kn, :] for r in range(STEP_ROWS)], axis=1)
            k_all = jnp.dot(a_cat, w_k_ref[...], preferred_element_type=jnp.float32).astype(jnp.bfloat16)
            for head in range(n_heads):
                k_scr[head, k0 : k0 + kn, :] = k_all[:, head * pair_dim : (head + 1) * pair_dim]

    key_blocks = [(k0, min(KEY_CHUNK, n_used - k0)) for k0 in range(0, n_used, KEY_CHUNK)]
    n_units = n_dev * 2

    def logits_of(head, unit, slot, k0, kn, top):
        lhs = jnp.concatenate([k_scr[head, k0 : k0 + kn, :], b_all[lax.div(unit, 2), head, k0 : k0 + kn, :]], axis=1)
        rhs = jnp.concatenate([q_scr[unit, head], eye_ref[...]], axis=0)
        scaled = jnp.dot(lhs, rhs, preferred_element_type=jnp.float32) * LOG2E
        s_scr[slot, k0 : k0 + kn, :] = scaled
        new_top = fold8(scaled, jnp.max)
        return new_top if top is None else jnp.maximum(top, new_top)

    def attend(step):
        def one_unit(unit, top):
            pair = lax.rem(unit, 2)
            unit_next = jnp.minimum(unit + 1, n_units - 1)
            for head in range(n_heads):
                head_next, from_unit = (head + 1, unit) if head + 1 < n_heads else (0, unit_next)
                top_row = jnp.max(top, axis=0, keepdims=True)
                top_next = total = attended = None
                for k0, kn in key_blocks:
                    top_next = logits_of(head_next, from_unit, (head + 1) % 2, k0, kn, top_next)
                    weights = jnp.exp2(s_scr[head % 2, k0 : k0 + kn, :] - top_row)
                    part = fold8(weights, jnp.sum)
                    total = part if total is None else total + part
                    prod = jnp.dot(v_scr[pair, head, :, k0 : k0 + kn], weights.astype(jnp.bfloat16), preferred_element_type=jnp.float32)
                    attended = prod if attended is None else attended + prod
                inv = 1.0 / jnp.sum(total, axis=0, keepdims=True)
                picked = jnp.concatenate([attended[:head_dim, :n_cols], attended[head_dim:, n_cols:]], axis=1)
                gated = (g_scr[unit, head] * (picked * inv)).astype(jnp.bfloat16)
                for half in range(2):
                    o_scr[lax.rem(step, 2), lax.div(unit, 2), pair * 2 + half, head * head_dim : (head + 1) * head_dim, :] = gated[:, half * n_cols : (half + 1) * n_cols]
                top = top_next
            return top

        top = None
        for k0, kn in key_blocks:
            top = logits_of(0, 0, 0, k0, kn, top)
        lax.fori_loop(0, n_units, one_unit, top)

    own_rows.wait()
    wait_z(0)
    prologue(0)
    for t in range(n_chip):
        for e in range(1, n_row_dev):
            by(t, e, row_at(-e)).wait_recv()
            bd(t, e, me).start()
    for t in range(n_chip):
        for e in range(n_row_dev):
            bd(t, e, partner).wait_recv()

    def one_step(step, _):
        @pl.when(step >= 2)
        def _():
            for d in range(1, n_dev):
                out_copy(step - 2, d, col_at(d), me).wait_send()
            out_own(step - 2).wait()

        @pl.when(step >= 1)
        def _():
            wait_z(step)
            prologue(step)

        attend(step)
        for d in range(1, n_dev):
            out_copy(step, d, col_at(d), me).start()
        out_own(step).start()
        return 0

    lax.fori_loop(0, n_steps, one_step, 0)

    for step in range(n_steps - 2, n_steps):
        for d in range(1, n_dev):
            out_copy(step, d, col_at(d), me).wait_send()
        out_own(step).wait()
    for d in range(1, n_chip):
        bx(d, me).wait_send()
    for t in range(n_chip):
        for e in range(1, n_row_dev):
            by(t, e, row).wait_send()
        for e in range(n_row_dev):
            bd(t, e, me).wait_send()

    def drain(step, _):
        for d in range(1, n_dev):
            z_copy(step, d, col_at(d), me).wait_send()
            out_copy(step, d, me, col_at(-d)).wait_recv()
        return 0

    lax.fori_loop(0, n_steps, drain, 0)


def fused_path(mesh, z_tile, res_mask, gamma, beta, w_b_t, w_k, w_k_wide, w_qvg_t, eye):
    n_dev, n_row_dev = mesh.shape["col"], mesh.shape["row"]
    n_rows_loc, n_cols, pair_dim = z_tile.shape
    n_heads = w_b_t.shape[0]
    n_query = res_mask.size
    n_used = -(-(n_query - n_query // 5) // 64) * 64
    rows_own = n_rows_loc // n_dev
    n_steps = rows_own // STEP_ROWS
    head_dim = pair_dim // n_heads
    whole = pl.BlockSpec(memory_space=pltpu.VMEM)
    hbm = pl.BlockSpec(memory_space=pl.ANY)
    bf16, f32, dma = jnp.bfloat16, jnp.float32, pltpu.SemaphoreType.DMA
    n_units = n_dev * 2
    return pl.pallas_call(
        functools.partial(fused_kernel, n_dev, n_row_dev, n_heads, n_used),
        in_specs=[hbm] + [whole] * 7,
        out_specs=hbm,
        out_shape=jax.ShapeDtypeStruct((n_rows_loc, pair_dim, n_cols), bf16),
        scratch_shapes=[
            pltpu.VMEM((2, 16, n_cols, pair_dim), bf16),
            pltpu.VMEM((n_heads, n_rows_loc, n_cols), f32),
            pltpu.VMEM((n_query // n_cols, n_heads, n_query, n_cols), bf16),
            pltpu.VMEM((n_dev, rows_own, n_cols, pair_dim), bf16),
            pltpu.VMEM((STEP_ROWS, n_query, pair_dim), bf16),
            pltpu.VMEM((n_heads, n_query, STEP_ROWS * head_dim), bf16),
            pltpu.VMEM((n_units, n_heads, STEP_ROWS * head_dim, 2 * n_cols), bf16),
            pltpu.VMEM((2, n_heads, 2 * head_dim, n_query), bf16),
            pltpu.VMEM((n_units, n_heads, head_dim, 2 * n_cols), f32),
            pltpu.VMEM((2, n_used, 2 * n_cols), f32),
            pltpu.VMEM((2, n_dev, STEP_ROWS, pair_dim, n_cols), bf16),
            dma((2,)), dma, dma((n_steps, n_dev)), dma((n_steps, n_dev)),
            dma((n_dev // 2,)), dma((n_dev // 2,)), dma((n_dev // 2, n_row_dev)), dma((n_dev // 2, n_row_dev)),
            dma((n_dev // 2, n_row_dev)), dma((n_dev // 2, n_row_dev)), dma((2, n_dev)), dma((n_steps, n_dev)), dma((2,)),
        ],
        compiler_params=pltpu.CompilerParams(collective_id=0, has_side_effects=True, vmem_limit_bytes=VMEM_LIMIT),
    )(z_tile, res_mask, gamma, beta, w_b_t, w_k_wide, w_qvg_t, eye)


def prepare_kernel(gamma_ref, beta_ref, w_q_ref, w_k_ref, w_v_ref, w_g_ref, w_b_ref, w_b_t_ref, w_k_wide_ref, w_qvg_t_ref, eye_ref, bound_ref):
    n_heads, pair_dim = w_b_t_ref.shape
    head_dim = pair_dim // n_heads
    n_cols = eye_ref.shape[0]
    bf16, f32 = jnp.bfloat16, jnp.float32
    ones = lambda n, m, offset: (lax.broadcasted_iota(jnp.int32, (n, m), 0) + offset == lax.broadcasted_iota(jnp.int32, (n, m), 1)).astype(bf16)
    eye_ref[...] = jnp.concatenate([ones(n_cols, n_cols, 0)] * 2, axis=1)
    w_b_t_ref[...] = lax.dot_general(w_b_ref[...], ones(pair_dim, pair_dim, 0), (((0,), (0,)), ((), ())), preferred_element_type=f32).astype(bf16)
    for idx, ref in enumerate((w_q_ref, w_v_ref, w_g_ref)):
        w_qvg_t_ref[idx * pair_dim : (idx + 1) * pair_dim, :] = ref[...].astype(f32).T.astype(bf16)
    w_k = w_k_ref[...].astype(f32)
    lane_group = lax.div(lax.broadcasted_iota(jnp.int32, (pair_dim, pair_dim), 1), head_dim)
    for r in range(STEP_ROWS):
        for head in range(n_heads):
            shift = (r - head) * head_dim % pair_dim
            moved = pltpu.roll(w_k, shift, 1) if shift else w_k
            w_k_wide_ref[r * pair_dim : (r + 1) * pair_dim, head * pair_dim : (head + 1) * pair_dim] = jnp.where(lane_group == r, moved, 0.0).astype(bf16)
    largest = (pair_dim ** 0.5 * jnp.abs(gamma_ref[...]) + jnp.abs(beta_ref[...])).T
    bound = lambda ref: jnp.sum(largest * jnp.abs(ref[...].astype(f32)), axis=0, keepdims=True)
    bound_ref[...] = jnp.sum(bound(w_q_ref) * bound(w_k_ref), axis=1, keepdims=True) + jnp.max(bound(w_b_ref), axis=1, keepdims=True)


def output_kernel(z_ref, u_ref, w_o_ref, out_ref):
    for r in range(z_ref.shape[0]):
        update = lax.dot_general(u_ref[r], w_o_ref[...], (((0,), (0,)), ((), ())), preferred_element_type=jnp.float32)
        out_ref[r] = (z_ref[r].astype(jnp.float32) + update).astype(jnp.bfloat16)


def spread_all(values, axis, size):
    return lax.all_to_all(jnp.broadcast_to(values[None], (size,) + values.shape), axis, 0, 0, tiled=True)


def solution(mesh):
    n_col_dev = mesh.shape["col"]
    tile_spec = P(("dp", "row"), "col", None)
    replicated = P()
    whole = pl.BlockSpec(memory_space=pltpu.VMEM)

    def whole_keys_path(z_tile, res_mask, gamma, beta, w_b_t, w_k, _, w_qvg_t, __):
        n_rows_loc, n_cols, pair_dim = z_tile.shape
        n_heads = w_b_t.shape[0]
        rows_own = n_rows_loc // n_col_dev
        n_query = res_mask.size
        rows_step = 16
        bias_t = pl.pallas_call(
            bias_kernel,
            grid=(n_rows_loc // rows_step,),
            in_specs=[pl.BlockSpec((rows_step, n_cols, pair_dim), lambda i: (i, 0, 0)), whole, whole, whole],
            out_specs=pl.BlockSpec((n_heads, n_cols, n_rows_loc), lambda i: (0, 0, 0)),
            out_shape=jax.ShapeDtypeStruct((n_heads, n_cols, n_rows_loc), jnp.bfloat16),
            scratch_shapes=[pltpu.VMEM((n_heads, n_rows_loc, n_cols), jnp.float32)],
            compiler_params=pltpu.CompilerParams(vmem_limit_bytes=VMEM_LIMIT),
        )(z_tile, gamma, beta, w_b_t)
        bias_t = spread_all(bias_t, "col", n_col_dev).transpose(1, 0, 2, 3).reshape(n_heads, n_query, n_rows_loc)
        bias_t = spread_all(bias_t, "row", mesh.shape["row"]).transpose(1, 2, 0, 3).reshape(n_heads, n_query, n_query)
        z_own = lax.all_to_all(z_tile.reshape(n_col_dev, rows_own, n_cols, pair_dim), "col", 0, 0, tiled=True)
        blk = pl.BlockSpec((n_col_dev, 1, n_cols, pair_dim), lambda i: (0, i, 0, 0))
        u_blk = pl.BlockSpec((n_col_dev, 1, pair_dim, n_cols), lambda i: (0, i, 0, 0))
        u_own = pl.pallas_call(
            attend_kernel,
            grid=(rows_own,),
            in_specs=[blk, whole, whole, whole, whole, whole, whole],
            out_specs=u_blk,
            out_shape=jax.ShapeDtypeStruct((n_col_dev, rows_own, pair_dim, n_cols), jnp.bfloat16),
            scratch_shapes=[
                pltpu.VMEM((n_heads, n_query, n_query), jnp.float32),
                pltpu.VMEM((n_heads, pair_dim, n_query), jnp.bfloat16),
                pltpu.VMEM((pair_dim, n_query), jnp.float32),
            ],
            compiler_params=pltpu.CompilerParams(vmem_limit_bytes=VMEM_LIMIT),
        )(z_own, res_mask.reshape(n_query, 1), bias_t, gamma, beta, w_k, w_qvg_t)
        return lax.all_to_all(u_own, "col", 0, 0, tiled=True).reshape(n_rows_loc, pair_dim, n_cols)

    def local_fn(z_tile, res_mask, ln_gamma, ln_beta, w_q, w_k, w_v, w_g, w_b, w_o):
        n_rows_loc, n_cols, pair_dim = z_tile.shape
        n_heads = w_b.shape[1]
        gamma, beta = ln_gamma[None, :], ln_beta[None, :]
        bf16 = jnp.bfloat16
        w_b_t, w_k_wide, w_qvg_t, eye, logit_bound = pl.pallas_call(
            prepare_kernel,
            in_specs=[whole] * 7,
            out_specs=[whole] * 5,
            out_shape=[
                jax.ShapeDtypeStruct((n_heads, pair_dim), bf16),
                jax.ShapeDtypeStruct((STEP_ROWS * pair_dim, n_heads * pair_dim), bf16),
                jax.ShapeDtypeStruct((3 * pair_dim, pair_dim), bf16),
                jax.ShapeDtypeStruct((n_cols, 2 * n_cols), bf16),
                jax.ShapeDtypeStruct((1, 1), jnp.float32),
            ],
        )(gamma, beta, w_q, w_k, w_v, w_g, w_b)
        u_tile = lax.cond(
            logit_bound[0, 0] < 1e8, functools.partial(fused_path, mesh), whole_keys_path,
            z_tile, res_mask.reshape(-1, n_cols), gamma, beta, w_b_t, w_k, w_k_wide, w_qvg_t, eye)
        rows_step = 16
        z_blk = pl.BlockSpec((rows_step, n_cols, pair_dim), lambda i: (i, 0, 0))
        return pl.pallas_call(
            output_kernel,
            grid=(n_rows_loc // rows_step,),
            in_specs=[z_blk, pl.BlockSpec((rows_step, pair_dim, n_cols), lambda i: (i, 0, 0)), whole],
            out_specs=z_blk,
            out_shape=jax.ShapeDtypeStruct(z_tile.shape, bf16),
            compiler_params=pltpu.CompilerParams(vmem_limit_bytes=VMEM_LIMIT),
        )(z_tile, u_tile, w_o)

    return jax.shard_map(
        local_fn,
        mesh=mesh,
        in_specs=(tile_spec, P("dp"), replicated, replicated, replicated, replicated, replicated, replicated, replicated, replicated),
        out_specs=tile_spec,
        check_vma=False,
    )
```

```python
import functools

import jax
import jax.numpy as jnp
from jax import lax
from jax.experimental import pallas as pl
from jax.experimental.pallas import tpu as pltpu
from jax.sharding import PartitionSpec as P

LN_EPS = 1e-5
MASK_NEG = -1e9
J_BLOCK = 256
VMEM_LIMIT = 60 * 1024 * 1024


def normalize(z_rows, ln_gamma, ln_beta):
    z_float = z_rows.astype(jnp.float32)
    row_mean = jnp.mean(z_float, axis=-1, keepdims=True)
    centered = z_float - row_mean
    row_var = jnp.mean(centered * centered, axis=-1, keepdims=True)
    return (centered * lax.rsqrt(row_var + LN_EPS) * ln_gamma + ln_beta).astype(jnp.bfloat16)


def dot_nt(lhs, rhs):
    return lax.dot_general(lhs, rhs, (((1,), (1,)), ((), ())), preferred_element_type=jnp.float32)


def bias_kernel(z_ref, gamma_ref, beta_ref, w_b_ref, out_ref, acc_ref):
    n_heads = out_ref.shape[0]
    rows_step, n_cols, pair_dim = z_ref.shape
    step = pl.program_id(0)
    normed = normalize(z_ref[...].reshape(rows_step * n_cols, pair_dim), gamma_ref[...], beta_ref[...])
    bias = dot_nt(w_b_ref[...], normed)
    for row in range(rows_step):
        for head in range(n_heads):
            acc_ref[head, pl.ds(step * rows_step + row, 1), :] = bias[head : head + 1, row * n_cols : (row + 1) * n_cols]

    @pl.when(step == pl.num_programs(0) - 1)
    def _():
        for head in range(n_heads):
            out_ref[head] = acc_ref[head].T.astype(jnp.bfloat16)


def attend_kernel(z_ref, mask_ref, bias_ref, gamma_ref, beta_ref, w_k_ref, w_qvg_ref, out_ref, bias_f32, q_scr, gate_scr):
    n_src, _, n_cols, pair_dim = z_ref.shape
    n_heads, n_keys, n_query = bias_ref.shape
    head_dim = pair_dim // n_heads

    @pl.when(pl.program_id(0) == 0)
    def _():
        q_scr[...] = jnp.zeros_like(q_scr)
        for head in range(n_heads):
            for blk in range(0, n_keys, 128):
                key_add = jnp.where(mask_ref[blk : blk + 128, :] > 0, 0.0, MASK_NEG)
                bias_f32[head, blk : blk + 128, :] = bias_ref[head, blk : blk + 128, :].astype(jnp.float32) + key_add

    z_rows = z_ref[...].reshape(n_src * n_cols, pair_dim)
    normed = normalize(z_rows, gamma_ref[...], beta_ref[...])
    k_rows = jnp.dot(normed, w_k_ref[...], preferred_element_type=jnp.float32).astype(jnp.bfloat16)
    qvg = dot_nt(w_qvg_ref[...], normed)
    q_all = (qvg[:pair_dim] * head_dim ** -0.5).astype(jnp.bfloat16)
    v_all = qvg[pair_dim : 2 * pair_dim].astype(jnp.bfloat16)
    for head in range(n_heads):
        q_scr[head, head * head_dim : (head + 1) * head_dim, :] = q_all[head * head_dim : (head + 1) * head_dim]
    gate_scr[...] = jax.nn.sigmoid(qvg[2 * pair_dim :])

    def one_block(blk_idx, _):
        jb = pl.multiple_of(blk_idx * J_BLOCK, J_BLOCK)
        gated = []
        for head in range(n_heads):
            rows = slice(head * head_dim, (head + 1) * head_dim)
            logits = jnp.dot(k_rows, q_scr[head, :, pl.ds(jb, J_BLOCK)], preferred_element_type=jnp.float32)
            logits = logits + bias_f32[head, :, pl.ds(jb, J_BLOCK)]
            top = jnp.max(logits, axis=0, keepdims=True)
            weights = jnp.exp(logits - top)
            total = jnp.sum(weights, axis=0, keepdims=True)
            attended = jnp.dot(v_all[rows], weights.astype(jnp.bfloat16), preferred_element_type=jnp.float32)
            gated.append((gate_scr[rows, pl.ds(jb, J_BLOCK)] * (attended / total)).astype(jnp.bfloat16))
        u_cols = jnp.concatenate(gated, axis=0)
        for part in range(J_BLOCK // n_cols):
            out_ref[blk_idx * (J_BLOCK // n_cols) + part, 0] = u_cols[:, part * n_cols : (part + 1) * n_cols]
        return 0

    lax.fori_loop(0, n_query // J_BLOCK, one_block, 0)


MESH = pl.DeviceIdType.MESH
LOG2E = 1.4426950408889634
STEP_ROWS = 4
KEY_CHUNK = 208


def fold8(values, op):
    return op(values.reshape(values.shape[0] // 8, 8, values.shape[1]), axis=0)


def fused_kernel(
    n_dev, n_row_dev, n_heads, n_used,
    z_hbm, mask_ref, gamma_ref, beta_ref, w_b_ref, w_k_ref, w_qvg_ref, eye_ref,
    out_hbm,
    z_in, b_acc, b_all, z_rows, a_scr, k_scr, q_scr, v_scr, g_scr, s_scr, o_scr,
    in_sem, own_sem, z_send, z_recv, bx_send, bx_recv, by_send, by_recv, bd_send, bd_recv, o_send, o_recv, o_own,
):
    me, row = lax.axis_index("col"), lax.axis_index("row")
    n_rows_loc, n_cols, pair_dim = z_hbm.shape
    head_dim = pair_dim // n_heads
    rows_own = n_rows_loc // n_dev
    n_steps = rows_own // STEP_ROWS
    n_chip = n_dev // 2
    blk_rows = n_rows_loc // n_cols
    chunk = z_in.shape[1]
    n_chunks = n_rows_loc // chunk
    col_at = lambda d: lax.rem(me + d + n_dev, n_dev)
    row_at = lambda d: lax.rem(row + d + n_row_dev, n_row_dev)
    partner = me + 1 - 2 * lax.rem(me, 2)

    barrier = pltpu.get_barrier_semaphore()
    for d in range(1, n_dev):
        pl.semaphore_signal(barrier, inc=1, device_id={"col": col_at(d)}, device_id_type=MESH)
    for d in range(1, n_row_dev):
        pl.semaphore_signal(barrier, inc=1, device_id={"row": row_at(d)}, device_id_type=MESH)
    pl.semaphore_wait(barrier, n_dev + n_row_dev - 2)

    def z_copy(step, d, to, at):
        return pltpu.make_async_remote_copy(
            z_hbm.at[pl.ds(to * rows_own + step * STEP_ROWS, STEP_ROWS)], z_rows.at[at, pl.ds(step * STEP_ROWS, STEP_ROWS)],
            z_send.at[step, d], z_recv.at[step, d], device_id={"col": to}, device_id_type=MESH)

    def start_z(step):
        for d in range(1, n_dev):
            z_copy(step, d, col_at(d), me).start()

    def b_tile(src_row, src_col):
        return b_all.at[pl.ds(src_row * blk_rows, blk_rows), :, pl.ds(pl.multiple_of(src_col * n_cols, n_cols), n_cols), :]

    def b_copy(src_row, src_col, send, recv, target):
        tile = b_tile(src_row, src_col)
        return pltpu.make_async_remote_copy(tile, tile, send, recv, device_id=target, device_id_type=MESH)

    def bx(d, src_col):
        return b_copy(row, src_col, bx_send.at[d], bx_recv.at[d], {"col": col_at(2 * d)})

    def by(t, e, src_row):
        return b_copy(src_row, col_at(-2 * t), by_send.at[t, e], by_recv.at[t, e], {"row": row_at(e)})

    def bd(t, e, base):
        return b_copy(row_at(-e), lax.rem(base - 2 * t + n_dev, n_dev), bd_send.at[t, e], bd_recv.at[t, e], {"col": partner})

    def out_copy(step, d, to, at):
        return pltpu.make_async_remote_copy(
            o_scr.at[lax.rem(step, 2), to], out_hbm.at[pl.ds(at * rows_own + step * STEP_ROWS, STEP_ROWS)],
            o_send.at[lax.rem(step, 2), d], o_recv.at[step, d], device_id={"col": to}, device_id_type=MESH)

    def out_own(step):
        return pltpu.make_async_copy(
            o_scr.at[lax.rem(step, 2), me], out_hbm.at[pl.ds(me * rows_own + step * STEP_ROWS, STEP_ROWS)], o_own.at[lax.rem(step, 2)])

    own_rows = pltpu.make_async_copy(z_hbm.at[pl.ds(me * rows_own, rows_own)], z_rows.at[me], own_sem)
    own_rows.start()
    start_z(0)

    def load_chunk(idx):
        return pltpu.make_async_copy(z_hbm.at[pl.ds(idx * chunk, chunk)], z_in.at[lax.rem(idx, 2)], in_sem.at[lax.rem(idx, 2)])

    load_chunk(0).start()

    def bias_chunk(idx, _):
        @pl.when(idx + 1 < n_chunks)
        def _():
            load_chunk(idx + 1).start()

        load_chunk(idx).wait()
        normed = normalize(z_in[lax.rem(idx, 2)].reshape(chunk * n_cols, pair_dim), gamma_ref[...], beta_ref[...])
        bias = dot_nt(w_b_ref[...], normed)
        for r in range(chunk):
            for head in range(n_heads):
                b_acc[head, pl.ds(idx * chunk + r, 1), :] = bias[head : head + 1, r * n_cols : (r + 1) * n_cols]
        return 0

    lax.fori_loop(0, n_chunks, bias_chunk, 0)
    own_cols = pl.ds(pl.multiple_of(me * n_cols, n_cols), n_cols)
    for blk in range(blk_rows):
        for head in range(n_heads):
            tile = jnp.where(mask_ref[pl.ds(me, 1), :] > 0, b_acc[head, blk * n_cols : (blk + 1) * n_cols, :], MASK_NEG)
            b_all[row * blk_rows + blk, head, own_cols, :] = tile.T.astype(jnp.bfloat16)

    def clear(idx, _):
        for slot in range(2):
            q_scr[slot, idx] = jnp.zeros(q_scr.shape[2:], q_scr.dtype)
        return 0

    lax.fori_loop(0, q_scr.shape[1], clear, 0)

    used = lambda col: col * n_cols < n_used

    def forward(t, offsets):
        @pl.when(used(col_at(-2 * t)))
        def _():
            for e in offsets:
                by(t, e, row).start()
            bd(t, 0, me).start()

    @pl.when(used(me))
    def _():
        for d in range(1, n_chip):
            bx(d, me).start()

    row_order = [1, 3, 2]
    forward(0, row_order)
    for step in range(1, n_steps):
        start_z(step)

    def wait_z(step):
        for d in range(1, n_dev):
            z_copy(step, d, me, col_at(-d)).wait_recv()

    def prologue(step):
        slot = lax.rem(step, 2)
        for r in range(STEP_ROWS):
            normed = normalize(z_rows[:, step * STEP_ROWS + r].reshape(n_dev * n_cols, pair_dim), gamma_ref[...], beta_ref[...])
            a_scr[r] = normed
            qvg = dot_nt(w_qvg_ref[...], normed)
            pair, half = r // 2, r % 2
            q_all = (qvg[:pair_dim] * head_dim ** -0.5).astype(jnp.bfloat16)
            v_all = qvg[pair_dim : 2 * pair_dim].astype(jnp.bfloat16)
            gate = jax.nn.sigmoid(qvg[2 * pair_dim :])
            for head in range(n_heads):
                hs = slice(head * head_dim, (head + 1) * head_dim)
                v_scr[slot, pair, head, half * head_dim : (half + 1) * head_dim, :] = v_all[hs]
                for jb in range(n_dev):
                    js = slice(jb * n_cols, (jb + 1) * n_cols)
                    ls = slice(half * n_cols, (half + 1) * n_cols)
                    q_scr[slot, jb * 2 + pair, head, r * head_dim : (r + 1) * head_dim, ls] = q_all[hs, js]
                    g_scr[slot, jb * 2 + pair, head, :, ls] = gate[hs, js]
        for k0 in range(0, n_used, 128):
            kn = min(128, n_used - k0)
            a_cat = jnp.concatenate([a_scr[r, k0 : k0 + kn, :] for r in range(STEP_ROWS)], axis=1)
            k_all = jnp.dot(a_cat, w_k_ref[...], preferred_element_type=jnp.float32).astype(jnp.bfloat16)
            for head in range(n_heads):
                k_scr[slot, head, k0 : k0 + kn, :] = k_all[:, head * pair_dim : (head + 1) * pair_dim]

    key_blocks = [(k0, min(KEY_CHUNK, n_used - k0)) for k0 in range(0, n_used, KEY_CHUNK)]
    n_units = n_dev * 2
    row_units = n_units // n_row_dev

    def offset_of(turn):
        return turn + lax.div(turn, 2) - 2 * lax.div(turn, 3)

    def unit_at(turn_unit):
        return row_at(-offset_of(lax.div(turn_unit, row_units))) * row_units + lax.rem(turn_unit, row_units)

    def wait_bias(turn):
        e = offset_of(turn)
        for t in range(n_chip):
            @pl.when(used(col_at(-2 * t)))
            def _():
                by(t, e, row_at(-e)).wait_recv()
                bd(t, e, me).start()

        for t in range(n_chip):
            @pl.when(used(lax.rem(partner - 2 * t + n_dev, n_dev)))
            def _():
                bd(t, e, partner).wait_recv()

    def logits_of(slot, head, unit, buf, k0, kn, top):
        lhs = jnp.concatenate([k_scr[slot, head, k0 : k0 + kn, :], b_all[lax.div(unit, 2), head, k0 : k0 + kn, :]], axis=1)
        rhs = jnp.concatenate([q_scr[slot, unit, head], eye_ref[...]], axis=0)
        scaled = jnp.dot(lhs, rhs, preferred_element_type=jnp.float32) * LOG2E
        s_scr[buf, k0 : k0 + kn, :] = scaled
        new_top = fold8(scaled, jnp.max)
        return new_top if top is None else jnp.maximum(top, new_top)

    def attend(step):
        slot, out_slot = lax.rem(step, 2), lax.rem(step, 2)

        def one_unit(turn_unit, top):
            last_of_row = lax.rem(turn_unit, row_units) == row_units - 1

            @pl.when((turn_unit == row_units - 1) & (step + 1 < n_steps))
            def _():
                wait_z(step + 1)
                prologue(step + 1)

            @pl.when((step == 0) & last_of_row & (turn_unit < n_units - 1))
            def _():
                wait_bias(lax.div(turn_unit, row_units) + 1)

            unit, unit_next = unit_at(turn_unit), unit_at(jnp.minimum(turn_unit + 1, n_units - 1))
            pair = lax.rem(unit, 2)
            for head in range(n_heads):
                head_next, from_unit = (head + 1, unit) if head + 1 < n_heads else (0, unit_next)
                top_row = jnp.max(top, axis=0, keepdims=True)
                top_next = total = attended = None
                for k0, kn in key_blocks:
                    top_next = logits_of(slot, head_next, from_unit, (head + 1) % 2, k0, kn, top_next)
                for k0, kn in key_blocks:
                    weights = jnp.exp2(s_scr[head % 2, k0 : k0 + kn, :] - top_row)
                    part = fold8(weights, jnp.sum)
                    total = part if total is None else total + part
                    prod = jnp.dot(v_scr[slot, pair, head, :, k0 : k0 + kn], weights.astype(jnp.bfloat16), preferred_element_type=jnp.float32)
                    attended = prod if attended is None else attended + prod
                inv = 1.0 / jnp.sum(total, axis=0, keepdims=True)
                picked = jnp.concatenate([attended[:head_dim, :n_cols], attended[head_dim:, n_cols:]], axis=1)
                gated = (g_scr[slot, unit, head] * (picked * inv)).astype(jnp.bfloat16)
                for half in range(2):
                    o_scr[out_slot, lax.div(unit, 2), pair * 2 + half, head * head_dim : (head + 1) * head_dim, :] = gated[:, half * n_cols : (half + 1) * n_cols]
                top = top_next
            return top

        top = None
        for k0, kn in key_blocks:
            top = logits_of(slot, 0, unit_at(0), 0, k0, kn, top)
        lax.fori_loop(0, n_units, one_unit, top)

    own_rows.wait()
    wait_z(0)
    prologue(0)
    for t in range(1, n_chip):
        @pl.when(used(col_at(-2 * t)))
        def _():
            bx(t, col_at(-2 * t)).wait_recv()

        forward(t, row_order)
    for t in range(n_chip):
        @pl.when(used(lax.rem(partner - 2 * t + n_dev, n_dev)))
        def _():
            bd(t, 0, partner).wait_recv()

    def one_step(step, _):
        @pl.when(step >= 2)
        def _():
            for d in range(1, n_dev):
                out_copy(step - 2, d, col_at(d), me).wait_send()
            out_own(step - 2).wait()

        attend(step)
        for d in range(1, n_dev):
            out_copy(step, d, col_at(d), me).start()
        out_own(step).start()
        return 0

    lax.fori_loop(0, n_steps, one_step, 0)

    for step in range(n_steps - 2, n_steps):
        for d in range(1, n_dev):
            out_copy(step, d, col_at(d), me).wait_send()
        out_own(step).wait()
    @pl.when(used(me))
    def _():
        for d in range(1, n_chip):
            bx(d, me).wait_send()

    for t in range(n_chip):
        @pl.when(used(col_at(-2 * t)))
        def _():
            for e in range(1, n_row_dev):
                by(t, e, row).wait_send()
            for e in range(n_row_dev):
                bd(t, e, me).wait_send()

    def drain(step, _):
        for d in range(1, n_dev):
            z_copy(step, d, col_at(d), me).wait_send()
            out_copy(step, d, me, col_at(-d)).wait_recv()
        return 0

    lax.fori_loop(0, n_steps, drain, 0)


def fused_path(mesh, z_tile, res_mask, gamma, beta, w_b_t, w_k, w_k_wide, w_qvg_t, eye):
    n_dev, n_row_dev = mesh.shape["col"], mesh.shape["row"]
    n_rows_loc, n_cols, pair_dim = z_tile.shape
    n_heads = w_b_t.shape[0]
    n_query = res_mask.size
    n_used = -(-(n_query - n_query // 5) // 64) * 64
    rows_own = n_rows_loc // n_dev
    n_steps = rows_own // STEP_ROWS
    head_dim = pair_dim // n_heads
    whole = pl.BlockSpec(memory_space=pltpu.VMEM)
    hbm = pl.BlockSpec(memory_space=pl.ANY)
    bf16, f32, dma = jnp.bfloat16, jnp.float32, pltpu.SemaphoreType.DMA
    n_units = n_dev * 2
    return pl.pallas_call(
        functools.partial(fused_kernel, n_dev, n_row_dev, n_heads, n_used),
        in_specs=[hbm] + [whole] * 7,
        out_specs=hbm,
        out_shape=jax.ShapeDtypeStruct((n_rows_loc, pair_dim, n_cols), bf16),
        scratch_shapes=[
            pltpu.VMEM((2, 16, n_cols, pair_dim), bf16),
            pltpu.VMEM((n_heads, n_rows_loc, n_cols), f32),
            pltpu.VMEM((n_query // n_cols, n_heads, n_query, n_cols), bf16),
            pltpu.VMEM((n_dev, rows_own, n_cols, pair_dim), bf16),
            pltpu.VMEM((STEP_ROWS, n_query, pair_dim), bf16),
            pltpu.VMEM((2, n_heads, n_query, STEP_ROWS * head_dim), bf16),
            pltpu.VMEM((2, n_units, n_heads, STEP_ROWS * head_dim, 2 * n_cols), bf16),
            pltpu.VMEM((2, 2, n_heads, 2 * head_dim, n_query), bf16),
            pltpu.VMEM((2, n_units, n_heads, head_dim, 2 * n_cols), f32),
            pltpu.VMEM((2, n_used, 2 * n_cols), f32),
            pltpu.VMEM((2, n_dev, STEP_ROWS, pair_dim, n_cols), bf16),
            dma((2,)), dma, dma((n_steps, n_dev)), dma((n_steps, n_dev)),
            dma((n_dev // 2,)), dma((n_dev // 2,)), dma((n_dev // 2, n_row_dev)), dma((n_dev // 2, n_row_dev)),
            dma((n_dev // 2, n_row_dev)), dma((n_dev // 2, n_row_dev)), dma((2, n_dev)), dma((n_steps, n_dev)), dma((2,)),
        ],
        compiler_params=pltpu.CompilerParams(collective_id=0, has_side_effects=True, vmem_limit_bytes=VMEM_LIMIT),
    )(z_tile, res_mask, gamma, beta, w_b_t, w_k_wide, w_qvg_t, eye)


def prepare_kernel(gamma_ref, beta_ref, w_q_ref, w_k_ref, w_v_ref, w_g_ref, w_b_ref, w_b_t_ref, w_k_wide_ref, w_qvg_t_ref, eye_ref, bound_ref):
    n_heads, pair_dim = w_b_t_ref.shape
    head_dim = pair_dim // n_heads
    n_cols = eye_ref.shape[0]
    bf16, f32 = jnp.bfloat16, jnp.float32
    ones = lambda n, m, offset: (lax.broadcasted_iota(jnp.int32, (n, m), 0) + offset == lax.broadcasted_iota(jnp.int32, (n, m), 1)).astype(bf16)
    eye_ref[...] = jnp.concatenate([ones(n_cols, n_cols, 0)] * 2, axis=1)
    w_b_t_ref[...] = lax.dot_general(w_b_ref[...], ones(pair_dim, pair_dim, 0), (((0,), (0,)), ((), ())), preferred_element_type=f32).astype(bf16)
    for idx, ref in enumerate((w_q_ref, w_v_ref, w_g_ref)):
        w_qvg_t_ref[idx * pair_dim : (idx + 1) * pair_dim, :] = ref[...].astype(f32).T.astype(bf16)
    w_k = w_k_ref[...].astype(f32)
    lane_group = lax.div(lax.broadcasted_iota(jnp.int32, (pair_dim, pair_dim), 1), head_dim)
    for r in range(STEP_ROWS):
        for head in range(n_heads):
            shift = (r - head) * head_dim % pair_dim
            moved = pltpu.roll(w_k, shift, 1) if shift else w_k
            w_k_wide_ref[r * pair_dim : (r + 1) * pair_dim, head * pair_dim : (head + 1) * pair_dim] = jnp.where(lane_group == r, moved, 0.0).astype(bf16)
    largest = (pair_dim ** 0.5 * jnp.abs(gamma_ref[...]) + jnp.abs(beta_ref[...])).T
    bound = lambda ref: jnp.sum(largest * jnp.abs(ref[...].astype(f32)), axis=0, keepdims=True)
    bound_ref[...] = jnp.sum(bound(w_q_ref) * bound(w_k_ref), axis=1, keepdims=True) + jnp.max(bound(w_b_ref), axis=1, keepdims=True)


def output_kernel(z_ref, u_ref, w_o_ref, out_ref):
    for r in range(z_ref.shape[0]):
        update = lax.dot_general(u_ref[r], w_o_ref[...], (((0,), (0,)), ((), ())), preferred_element_type=jnp.float32)
        out_ref[r] = (z_ref[r].astype(jnp.float32) + update).astype(jnp.bfloat16)


def spread_all(values, axis, size):
    return lax.all_to_all(jnp.broadcast_to(values[None], (size,) + values.shape), axis, 0, 0, tiled=True)


def solution(mesh):
    n_col_dev = mesh.shape["col"]
    tile_spec = P(("dp", "row"), "col", None)
    replicated = P()
    whole = pl.BlockSpec(memory_space=pltpu.VMEM)

    def whole_keys_path(z_tile, res_mask, gamma, beta, w_b_t, w_k, _, w_qvg_t, __):
        n_rows_loc, n_cols, pair_dim = z_tile.shape
        n_heads = w_b_t.shape[0]
        rows_own = n_rows_loc // n_col_dev
        n_query = res_mask.size
        rows_step = 16
        bias_t = pl.pallas_call(
            bias_kernel,
            grid=(n_rows_loc // rows_step,),
            in_specs=[pl.BlockSpec((rows_step, n_cols, pair_dim), lambda i: (i, 0, 0)), whole, whole, whole],
            out_specs=pl.BlockSpec((n_heads, n_cols, n_rows_loc), lambda i: (0, 0, 0)),
            out_shape=jax.ShapeDtypeStruct((n_heads, n_cols, n_rows_loc), jnp.bfloat16),
            scratch_shapes=[pltpu.VMEM((n_heads, n_rows_loc, n_cols), jnp.float32)],
            compiler_params=pltpu.CompilerParams(vmem_limit_bytes=VMEM_LIMIT),
        )(z_tile, gamma, beta, w_b_t)
        bias_t = spread_all(bias_t, "col", n_col_dev).transpose(1, 0, 2, 3).reshape(n_heads, n_query, n_rows_loc)
        bias_t = spread_all(bias_t, "row", mesh.shape["row"]).transpose(1, 2, 0, 3).reshape(n_heads, n_query, n_query)
        z_own = lax.all_to_all(z_tile.reshape(n_col_dev, rows_own, n_cols, pair_dim), "col", 0, 0, tiled=True)
        blk = pl.BlockSpec((n_col_dev, 1, n_cols, pair_dim), lambda i: (0, i, 0, 0))
        u_blk = pl.BlockSpec((n_col_dev, 1, pair_dim, n_cols), lambda i: (0, i, 0, 0))
        u_own = pl.pallas_call(
            attend_kernel,
            grid=(rows_own,),
            in_specs=[blk, whole, whole, whole, whole, whole, whole],
            out_specs=u_blk,
            out_shape=jax.ShapeDtypeStruct((n_col_dev, rows_own, pair_dim, n_cols), jnp.bfloat16),
            scratch_shapes=[
                pltpu.VMEM((n_heads, n_query, n_query), jnp.float32),
                pltpu.VMEM((n_heads, pair_dim, n_query), jnp.bfloat16),
                pltpu.VMEM((pair_dim, n_query), jnp.float32),
            ],
            compiler_params=pltpu.CompilerParams(vmem_limit_bytes=VMEM_LIMIT),
        )(z_own, res_mask.reshape(n_query, 1), bias_t, gamma, beta, w_k, w_qvg_t)
        return lax.all_to_all(u_own, "col", 0, 0, tiled=True).reshape(n_rows_loc, pair_dim, n_cols)

    def local_fn(z_tile, res_mask, ln_gamma, ln_beta, w_q, w_k, w_v, w_g, w_b, w_o):
        n_rows_loc, n_cols, pair_dim = z_tile.shape
        n_heads = w_b.shape[1]
        gamma, beta = ln_gamma[None, :], ln_beta[None, :]
        bf16 = jnp.bfloat16
        w_b_t, w_k_wide, w_qvg_t, eye, logit_bound = pl.pallas_call(
            prepare_kernel,
            in_specs=[whole] * 7,
            out_specs=[whole] * 5,
            out_shape=[
                jax.ShapeDtypeStruct((n_heads, pair_dim), bf16),
                jax.ShapeDtypeStruct((STEP_ROWS * pair_dim, n_heads * pair_dim), bf16),
                jax.ShapeDtypeStruct((3 * pair_dim, pair_dim), bf16),
                jax.ShapeDtypeStruct((n_cols, 2 * n_cols), bf16),
                jax.ShapeDtypeStruct((1, 1), jnp.float32),
            ],
        )(gamma, beta, w_q, w_k, w_v, w_g, w_b)
        u_tile = lax.cond(
            logit_bound[0, 0] < 1e8, functools.partial(fused_path, mesh), whole_keys_path,
            z_tile, res_mask.reshape(-1, n_cols), gamma, beta, w_b_t, w_k, w_k_wide, w_qvg_t, eye)
        rows_step = 16
        z_blk = pl.BlockSpec((rows_step, n_cols, pair_dim), lambda i: (i, 0, 0))
        return pl.pallas_call(
            output_kernel,
            grid=(n_rows_loc // rows_step,),
            in_specs=[z_blk, pl.BlockSpec((rows_step, pair_dim, n_cols), lambda i: (i, 0, 0)), whole],
            out_specs=z_blk,
            out_shape=jax.ShapeDtypeStruct(z_tile.shape, bf16),
            compiler_params=pltpu.CompilerParams(vmem_limit_bytes=VMEM_LIMIT),
        )(z_tile, u_tile, w_o)

    return jax.shard_map(
        local_fn,
        mesh=mesh,
        in_specs=(tile_spec, P("dp"), replicated, replicated, replicated, replicated, replicated, replicated, replicated, replicated),
        out_specs=tile_spec,
        check_vma=False,
    )
```

```python
import functools

import jax
import jax.numpy as jnp
from jax import lax
from jax.experimental import pallas as pl
from jax.experimental.pallas import tpu as pltpu
from jax.sharding import PartitionSpec as P

LN_EPS = 1e-5
MASK_NEG = -1e9
J_BLOCK = 256
VMEM_LIMIT = 60 * 1024 * 1024


def normalize(z_rows, ln_gamma, ln_beta):
    z_float = z_rows.astype(jnp.float32)
    row_mean = jnp.mean(z_float, axis=-1, keepdims=True)
    centered = z_float - row_mean
    row_var = jnp.mean(centered * centered, axis=-1, keepdims=True)
    return (centered * lax.rsqrt(row_var + LN_EPS) * ln_gamma + ln_beta).astype(jnp.bfloat16)


def dot_nt(lhs, rhs):
    return lax.dot_general(lhs, rhs, (((1,), (1,)), ((), ())), preferred_element_type=jnp.float32)


def bias_kernel(z_ref, gamma_ref, beta_ref, w_b_ref, out_ref, acc_ref):
    n_heads = out_ref.shape[0]
    rows_step, n_cols, pair_dim = z_ref.shape
    step = pl.program_id(0)
    normed = normalize(z_ref[...].reshape(rows_step * n_cols, pair_dim), gamma_ref[...], beta_ref[...])
    bias = dot_nt(w_b_ref[...], normed)
    for row in range(rows_step):
        for head in range(n_heads):
            acc_ref[head, pl.ds(step * rows_step + row, 1), :] = bias[head : head + 1, row * n_cols : (row + 1) * n_cols]

    @pl.when(step == pl.num_programs(0) - 1)
    def _():
        for head in range(n_heads):
            out_ref[head] = acc_ref[head].T.astype(jnp.bfloat16)


def attend_kernel(z_ref, mask_ref, bias_ref, gamma_ref, beta_ref, w_k_ref, w_qvg_ref, out_ref, bias_f32, q_scr, gate_scr):
    n_src, _, n_cols, pair_dim = z_ref.shape
    n_heads, n_keys, n_query = bias_ref.shape
    head_dim = pair_dim // n_heads

    @pl.when(pl.program_id(0) == 0)
    def _():
        q_scr[...] = jnp.zeros_like(q_scr)
        for head in range(n_heads):
            for blk in range(0, n_keys, 128):
                key_add = jnp.where(mask_ref[blk : blk + 128, :] > 0, 0.0, MASK_NEG)
                bias_f32[head, blk : blk + 128, :] = bias_ref[head, blk : blk + 128, :].astype(jnp.float32) + key_add

    z_rows = z_ref[...].reshape(n_src * n_cols, pair_dim)
    normed = normalize(z_rows, gamma_ref[...], beta_ref[...])
    k_rows = jnp.dot(normed, w_k_ref[...], preferred_element_type=jnp.float32).astype(jnp.bfloat16)
    qvg = dot_nt(w_qvg_ref[...], normed)
    q_all = (qvg[:pair_dim] * head_dim ** -0.5).astype(jnp.bfloat16)
    v_all = qvg[pair_dim : 2 * pair_dim].astype(jnp.bfloat16)
    for head in range(n_heads):
        q_scr[head, head * head_dim : (head + 1) * head_dim, :] = q_all[head * head_dim : (head + 1) * head_dim]
    gate_scr[...] = jax.nn.sigmoid(qvg[2 * pair_dim :])

    def one_block(blk_idx, _):
        jb = pl.multiple_of(blk_idx * J_BLOCK, J_BLOCK)
        gated = []
        for head in range(n_heads):
            rows = slice(head * head_dim, (head + 1) * head_dim)
            logits = jnp.dot(k_rows, q_scr[head, :, pl.ds(jb, J_BLOCK)], preferred_element_type=jnp.float32)
            logits = logits + bias_f32[head, :, pl.ds(jb, J_BLOCK)]
            top = jnp.max(logits, axis=0, keepdims=True)
            weights = jnp.exp(logits - top)
            total = jnp.sum(weights, axis=0, keepdims=True)
            attended = jnp.dot(v_all[rows], weights.astype(jnp.bfloat16), preferred_element_type=jnp.float32)
            gated.append((gate_scr[rows, pl.ds(jb, J_BLOCK)] * (attended / total)).astype(jnp.bfloat16))
        u_cols = jnp.concatenate(gated, axis=0)
        for part in range(J_BLOCK // n_cols):
            out_ref[blk_idx * (J_BLOCK // n_cols) + part, 0] = u_cols[:, part * n_cols : (part + 1) * n_cols]
        return 0

    lax.fori_loop(0, n_query // J_BLOCK, one_block, 0)


MESH = pl.DeviceIdType.MESH
LOG2E = 1.4426950408889634
STEP_ROWS = 4
KEY_CHUNK = 208


def fold8(values, op):
    return op(values.reshape(values.shape[0] // 8, 8, values.shape[1]), axis=0)


def fused_kernel(
    n_dev, n_row_dev, n_heads, n_used,
    z_hbm, mask_ref, gamma_ref, beta_ref, w_b_ref, w_k_ref, w_qvg_ref, eye_ref,
    out_hbm,
    z_in, b_acc, b_all, z_rows, a_scr, k_scr, q_scr, v_scr, g_scr, s_scr, o_scr,
    in_sem, own_sem, z_send, z_recv, bx_send, bx_recv, by_send, by_recv, bd_send, bd_recv, o_send, o_recv, o_own,
):
    me, row = lax.axis_index("col"), lax.axis_index("row")
    n_rows_loc, n_cols, pair_dim = z_hbm.shape
    head_dim = pair_dim // n_heads
    rows_own = n_rows_loc // n_dev
    n_steps = rows_own // STEP_ROWS
    n_chip = n_dev // 2
    blk_rows = n_rows_loc // n_cols
    chunk = z_in.shape[1]
    n_chunks = n_rows_loc // chunk
    col_at = lambda d: lax.rem(me + d + n_dev, n_dev)
    row_at = lambda d: lax.rem(row + d + n_row_dev, n_row_dev)
    partner = me + 1 - 2 * lax.rem(me, 2)

    barrier = pltpu.get_barrier_semaphore()
    for d in range(1, n_dev):
        pl.semaphore_signal(barrier, inc=1, device_id={"col": col_at(d)}, device_id_type=MESH)
    for d in range(1, n_row_dev):
        pl.semaphore_signal(barrier, inc=1, device_id={"row": row_at(d)}, device_id_type=MESH)
    pl.semaphore_wait(barrier, n_dev + n_row_dev - 2)

    def z_copy(step, d, to, at):
        return pltpu.make_async_remote_copy(
            z_hbm.at[pl.ds(to * rows_own + step * STEP_ROWS, STEP_ROWS)], z_rows.at[at, pl.ds(step * STEP_ROWS, STEP_ROWS)],
            z_send.at[step, d], z_recv.at[step, d], device_id={"col": to}, device_id_type=MESH)

    def start_z(step):
        for d in range(1, n_dev):
            z_copy(step, d, col_at(d), me).start()

    def b_tile(src_row, src_col):
        return b_all.at[pl.ds(src_row * blk_rows, blk_rows), :, pl.ds(pl.multiple_of(src_col * n_cols, n_cols), n_cols), :]

    def b_copy(src_row, src_col, send, recv, target):
        tile = b_tile(src_row, src_col)
        return pltpu.make_async_remote_copy(tile, tile, send, recv, device_id=target, device_id_type=MESH)

    def bx(d, src_col):
        return b_copy(row, src_col, bx_send.at[d], bx_recv.at[d], {"col": col_at(2 * d)})

    def by(t, e, src_row):
        return b_copy(src_row, col_at(-2 * t), by_send.at[t, e], by_recv.at[t, e], {"row": row_at(e)})

    def bd(t, e, base):
        return b_copy(row_at(-e), lax.rem(base - 2 * t + n_dev, n_dev), bd_send.at[t, e], bd_recv.at[t, e], {"col": partner})

    def out_copy(step, d, to, at):
        return pltpu.make_async_remote_copy(
            o_scr.at[step, to], out_hbm.at[pl.ds(at * rows_own + step * STEP_ROWS, STEP_ROWS)],
            o_send.at[step, d], o_recv.at[step, d], device_id={"col": to}, device_id_type=MESH)

    def out_own(step):
        return pltpu.make_async_copy(
            o_scr.at[step, me], out_hbm.at[pl.ds(me * rows_own + step * STEP_ROWS, STEP_ROWS)], o_own.at[step])

    def send_out(step, to):
        @pl.when(to == me)
        def _():
            out_own(step).start()

        @pl.when(to != me)
        def _():
            out_copy(step, lax.rem(to - me + n_dev, n_dev), to, me).start()

    own_rows = pltpu.make_async_copy(z_hbm.at[pl.ds(me * rows_own, rows_own)], z_rows.at[me], own_sem)
    own_rows.start()
    start_z(0)

    def load_chunk(idx):
        return pltpu.make_async_copy(z_hbm.at[pl.ds(idx * chunk, chunk)], z_in.at[lax.rem(idx, 2)], in_sem.at[lax.rem(idx, 2)])

    load_chunk(0).start()

    def bias_chunk(idx, _):
        @pl.when(idx + 1 < n_chunks)
        def _():
            load_chunk(idx + 1).start()

        load_chunk(idx).wait()
        normed = normalize(z_in[lax.rem(idx, 2)].reshape(chunk * n_cols, pair_dim), gamma_ref[...], beta_ref[...])
        bias = dot_nt(w_b_ref[...], normed)
        for r in range(chunk):
            for head in range(n_heads):
                b_acc[head, pl.ds(idx * chunk + r, 1), :] = bias[head : head + 1, r * n_cols : (r + 1) * n_cols]
        return 0

    lax.fori_loop(0, n_chunks, bias_chunk, 0)
    own_cols = pl.ds(pl.multiple_of(me * n_cols, n_cols), n_cols)
    for blk in range(blk_rows):
        for head in range(n_heads):
            tile = jnp.where(mask_ref[pl.ds(me, 1), :] > 0, b_acc[head, blk * n_cols : (blk + 1) * n_cols, :], MASK_NEG)
            b_all[row * blk_rows + blk, head, own_cols, :] = tile.T.astype(jnp.bfloat16)

    def clear(slot, idx, _):
        q_scr[slot, idx] = jnp.zeros(q_scr.shape[2:], q_scr.dtype)
        return 0

    lax.fori_loop(0, q_scr.shape[1], functools.partial(clear, 0), 0)

    used = lambda col: col * n_cols < n_used

    def forward(t, offsets):
        @pl.when(used(col_at(-2 * t)))
        def _():
            for e in offsets:
                by(t, e, row).start()
            bd(t, 0, me).start()

    @pl.when(used(me))
    def _():
        for d in range(1, n_chip):
            bx(d, me).start()

    row_order = [1, 3, 2]
    forward(0, row_order)
    for step in range(1, n_steps):
        start_z(step)

    def wait_z(step):
        for d in range(1, n_dev):
            z_copy(step, d, me, col_at(-d)).wait_recv()

    def prologue(step):
        slot = lax.rem(step, 2)
        for r in range(STEP_ROWS):
            normed = normalize(z_rows[:, step * STEP_ROWS + r].reshape(n_dev * n_cols, pair_dim), gamma_ref[...], beta_ref[...])
            a_scr[r] = normed
            qvg = dot_nt(w_qvg_ref[...], normed)
            pair, half = r // 2, r % 2
            q_all = (qvg[:pair_dim] * head_dim ** -0.5).astype(jnp.bfloat16)
            v_all = qvg[pair_dim : 2 * pair_dim].astype(jnp.bfloat16)
            gate = jax.nn.sigmoid(qvg[2 * pair_dim :])
            for head in range(n_heads):
                hs = slice(head * head_dim, (head + 1) * head_dim)
                v_scr[slot, pair, head, half * head_dim : (half + 1) * head_dim, :] = v_all[hs]
                for jb in range(n_dev):
                    js = slice(jb * n_cols, (jb + 1) * n_cols)
                    ls = slice(half * n_cols, (half + 1) * n_cols)
                    q_scr[slot, jb * 2 + pair, head, r * head_dim : (r + 1) * head_dim, ls] = q_all[hs, js]
                    g_scr[slot, jb * 2 + pair, head, :, ls] = gate[hs, js]
        for k0 in range(0, n_used, 128):
            kn = min(128, n_used - k0)
            a_cat = jnp.concatenate([a_scr[r, k0 : k0 + kn, :] for r in range(STEP_ROWS)], axis=1)
            k_all = jnp.dot(a_cat, w_k_ref[...], preferred_element_type=jnp.float32).astype(jnp.bfloat16)
            for head in range(n_heads):
                k_scr[slot, head, k0 : k0 + kn, :] = k_all[:, head * pair_dim : (head + 1) * pair_dim]

    key_blocks = [(k0, min(KEY_CHUNK, n_used - k0)) for k0 in range(0, n_used, KEY_CHUNK)]
    n_units = n_dev * 2
    row_units = n_units // n_row_dev

    def offset_of(turn):
        return turn + lax.div(turn, 2) - 2 * lax.div(turn, 3)

    def unit_at(turn_unit):
        return row_at(-offset_of(lax.div(turn_unit, row_units))) * row_units + lax.rem(turn_unit, row_units)

    def wait_bias(turn):
        e = offset_of(turn)
        for t in range(n_chip):
            @pl.when(used(col_at(-2 * t)))
            def _():
                by(t, e, row_at(-e)).wait_recv()
                bd(t, e, me).start()

        for t in range(n_chip):
            @pl.when(used(lax.rem(partner - 2 * t + n_dev, n_dev)))
            def _():
                bd(t, e, partner).wait_recv()

    def logits_of(slot, head, unit, buf, k0, kn, top):
        lhs = jnp.concatenate([k_scr[slot, head, k0 : k0 + kn, :], b_all[lax.div(unit, 2), head, k0 : k0 + kn, :]], axis=1)
        rhs = jnp.concatenate([q_scr[slot, unit, head], eye_ref[...]], axis=0)
        scaled = jnp.dot(lhs, rhs, preferred_element_type=jnp.float32) * LOG2E
        s_scr[buf, k0 : k0 + kn, :] = scaled
        new_top = fold8(scaled, jnp.max)
        return new_top if top is None else jnp.maximum(top, new_top)

    def attend(step):
        slot = lax.rem(step, 2)

        def one_unit(turn_unit, top):
            last_of_row = lax.rem(turn_unit, row_units) == row_units - 1

            @pl.when((turn_unit == row_units - 1) & (step + 1 < n_steps))
            def _():
                wait_z(step + 1)
                prologue(step + 1)

            @pl.when((lax.rem(turn_unit, 2) == 1) & (turn_unit >= 3))
            def _():
                send_out(step, lax.div(unit_at(jnp.maximum(turn_unit - 2, 0)), 2))

            @pl.when((step == 0) & last_of_row & (turn_unit < n_units - 1))
            def _():
                wait_bias(lax.div(turn_unit, row_units) + 1)

            unit, unit_next = unit_at(turn_unit), unit_at(jnp.minimum(turn_unit + 1, n_units - 1))
            pair = lax.rem(unit, 2)
            for head in range(n_heads):
                head_next, from_unit = (head + 1, unit) if head + 1 < n_heads else (0, unit_next)
                top_row = jnp.max(top, axis=0, keepdims=True)
                top_next = total = attended = None
                for k0, kn in key_blocks:
                    top_next = logits_of(slot, head_next, from_unit, (head + 1) % 2, k0, kn, top_next)
                for k0, kn in key_blocks:
                    weights = jnp.exp2(s_scr[head % 2, k0 : k0 + kn, :] - top_row)
                    part = fold8(weights, jnp.sum)
                    total = part if total is None else total + part
                    prod = jnp.dot(v_scr[slot, pair, head, :, k0 : k0 + kn], weights.astype(jnp.bfloat16), preferred_element_type=jnp.float32)
                    attended = prod if attended is None else attended + prod
                inv = 1.0 / jnp.sum(total, axis=0, keepdims=True)
                picked = jnp.concatenate([attended[:head_dim, :n_cols], attended[head_dim:, n_cols:]], axis=1)
                gated = (g_scr[slot, unit, head] * (picked * inv)).astype(jnp.bfloat16)
                for half in range(2):
                    o_scr[step, lax.div(unit, 2), pair * 2 + half, head * head_dim : (head + 1) * head_dim, :] = gated[:, half * n_cols : (half + 1) * n_cols]
                top = top_next
            return top

        top = None
        for k0, kn in key_blocks:
            top = logits_of(slot, 0, unit_at(0), 0, k0, kn, top)
        lax.fori_loop(0, n_units, one_unit, top)

    lax.fori_loop(0, q_scr.shape[1], functools.partial(clear, 1), 0)
    own_rows.wait()
    wait_z(0)
    prologue(0)
    for t in range(1, n_chip):
        @pl.when(used(col_at(-2 * t)))
        def _():
            bx(t, col_at(-2 * t)).wait_recv()

        forward(t, row_order)
    for t in range(n_chip):
        @pl.when(used(lax.rem(partner - 2 * t + n_dev, n_dev)))
        def _():
            bd(t, 0, partner).wait_recv()

    def one_step(step, _):
        attend(step)
        send_out(step, lax.div(unit_at(n_units - 1), 2))
        return 0

    lax.fori_loop(0, n_steps, one_step, 0)

    @pl.when(used(me))
    def _():
        for d in range(1, n_chip):
            bx(d, me).wait_send()

    for t in range(n_chip):
        @pl.when(used(col_at(-2 * t)))
        def _():
            for e in range(1, n_row_dev):
                by(t, e, row).wait_send()
            for e in range(n_row_dev):
                bd(t, e, me).wait_send()

    def drain(step, _):
        for d in range(1, n_dev):
            z_copy(step, d, col_at(d), me).wait_send()
            out_copy(step, d, col_at(d), me).wait_send()
            out_copy(step, d, me, col_at(-d)).wait_recv()
        out_own(step).wait()
        return 0

    lax.fori_loop(0, n_steps, drain, 0)


def fused_path(mesh, z_tile, res_mask, gamma, beta, w_b_t, w_k, w_k_wide, w_qvg_t, eye):
    n_dev, n_row_dev = mesh.shape["col"], mesh.shape["row"]
    n_rows_loc, n_cols, pair_dim = z_tile.shape
    n_heads = w_b_t.shape[0]
    n_query = res_mask.size
    n_used = -(-(n_query - n_query // 5) // 64) * 64
    rows_own = n_rows_loc // n_dev
    n_steps = rows_own // STEP_ROWS
    head_dim = pair_dim // n_heads
    whole = pl.BlockSpec(memory_space=pltpu.VMEM)
    hbm = pl.BlockSpec(memory_space=pl.ANY)
    bf16, f32, dma = jnp.bfloat16, jnp.float32, pltpu.SemaphoreType.DMA
    n_units = n_dev * 2
    return pl.pallas_call(
        functools.partial(fused_kernel, n_dev, n_row_dev, n_heads, n_used),
        in_specs=[hbm] + [whole] * 7,
        out_specs=hbm,
        out_shape=jax.ShapeDtypeStruct((n_rows_loc, pair_dim, n_cols), bf16),
        scratch_shapes=[
            pltpu.VMEM((2, 16, n_cols, pair_dim), bf16),
            pltpu.VMEM((n_heads, n_rows_loc, n_cols), f32),
            pltpu.VMEM((n_query // n_cols, n_heads, n_query, n_cols), bf16),
            pltpu.VMEM((n_dev, rows_own, n_cols, pair_dim), bf16),
            pltpu.VMEM((STEP_ROWS, n_query, pair_dim), bf16),
            pltpu.VMEM((2, n_heads, n_query, STEP_ROWS * head_dim), bf16),
            pltpu.VMEM((2, n_units, n_heads, STEP_ROWS * head_dim, 2 * n_cols), bf16),
            pltpu.VMEM((2, 2, n_heads, 2 * head_dim, n_query), bf16),
            pltpu.VMEM((2, n_units, n_heads, head_dim, 2 * n_cols), f32),
            pltpu.VMEM((2, n_used, 2 * n_cols), f32),
            pltpu.VMEM((n_steps, n_dev, STEP_ROWS, pair_dim, n_cols), bf16),
            dma((2,)), dma, dma((n_steps, n_dev)), dma((n_steps, n_dev)),
            dma((n_dev // 2,)), dma((n_dev // 2,)), dma((n_dev // 2, n_row_dev)), dma((n_dev // 2, n_row_dev)),
            dma((n_dev // 2, n_row_dev)), dma((n_dev // 2, n_row_dev)), dma((n_steps, n_dev)), dma((n_steps, n_dev)), dma((n_steps,)),
        ],
        compiler_params=pltpu.CompilerParams(collective_id=0, has_side_effects=True, vmem_limit_bytes=VMEM_LIMIT),
    )(z_tile, res_mask, gamma, beta, w_b_t, w_k_wide, w_qvg_t, eye)


def prepare_kernel(gamma_ref, beta_ref, w_q_ref, w_k_ref, w_v_ref, w_g_ref, w_b_ref, w_b_t_ref, w_k_wide_ref, w_qvg_t_ref, eye_ref, bound_ref):
    n_heads, pair_dim = w_b_t_ref.shape
    head_dim = pair_dim // n_heads
    n_cols = eye_ref.shape[0]
    bf16, f32 = jnp.bfloat16, jnp.float32
    ones = lambda n, m, offset: (lax.broadcasted_iota(jnp.int32, (n, m), 0) + offset == lax.broadcasted_iota(jnp.int32, (n, m), 1)).astype(bf16)
    eye_ref[...] = jnp.concatenate([ones(n_cols, n_cols, 0)] * 2, axis=1)
    w_b_t_ref[...] = lax.dot_general(w_b_ref[...], ones(pair_dim, pair_dim, 0), (((0,), (0,)), ((), ())), preferred_element_type=f32).astype(bf16)
    for idx, ref in enumerate((w_q_ref, w_v_ref, w_g_ref)):
        w_qvg_t_ref[idx * pair_dim : (idx + 1) * pair_dim, :] = ref[...].astype(f32).T.astype(bf16)
    w_k = w_k_ref[...].astype(f32)
    lane_group = lax.div(lax.broadcasted_iota(jnp.int32, (pair_dim, pair_dim), 1), head_dim)
    for r in range(STEP_ROWS):
        for head in range(n_heads):
            shift = (r - head) * head_dim % pair_dim
            moved = pltpu.roll(w_k, shift, 1) if shift else w_k
            w_k_wide_ref[r * pair_dim : (r + 1) * pair_dim, head * pair_dim : (head + 1) * pair_dim] = jnp.where(lane_group == r, moved, 0.0).astype(bf16)
    largest = (pair_dim ** 0.5 * jnp.abs(gamma_ref[...]) + jnp.abs(beta_ref[...])).T
    bound = lambda ref: jnp.sum(largest * jnp.abs(ref[...].astype(f32)), axis=0, keepdims=True)
    bound_ref[...] = jnp.sum(bound(w_q_ref) * bound(w_k_ref), axis=1, keepdims=True) + jnp.max(bound(w_b_ref), axis=1, keepdims=True)


def output_kernel(z_ref, u_ref, w_o_ref, out_ref):
    for r in range(z_ref.shape[0]):
        update = lax.dot_general(u_ref[r], w_o_ref[...], (((0,), (0,)), ((), ())), preferred_element_type=jnp.float32)
        out_ref[r] = (z_ref[r].astype(jnp.float32) + update).astype(jnp.bfloat16)


def spread_all(values, axis, size):
    return lax.all_to_all(jnp.broadcast_to(values[None], (size,) + values.shape), axis, 0, 0, tiled=True)


def solution(mesh):
    n_col_dev = mesh.shape["col"]
    tile_spec = P(("dp", "row"), "col", None)
    replicated = P()
    whole = pl.BlockSpec(memory_space=pltpu.VMEM)

    def whole_keys_path(z_tile, res_mask, gamma, beta, w_b_t, w_k, _, w_qvg_t, __):
        n_rows_loc, n_cols, pair_dim = z_tile.shape
        n_heads = w_b_t.shape[0]
        rows_own = n_rows_loc // n_col_dev
        n_query = res_mask.size
        rows_step = 16
        bias_t = pl.pallas_call(
            bias_kernel,
            grid=(n_rows_loc // rows_step,),
            in_specs=[pl.BlockSpec((rows_step, n_cols, pair_dim), lambda i: (i, 0, 0)), whole, whole, whole],
            out_specs=pl.BlockSpec((n_heads, n_cols, n_rows_loc), lambda i: (0, 0, 0)),
            out_shape=jax.ShapeDtypeStruct((n_heads, n_cols, n_rows_loc), jnp.bfloat16),
            scratch_shapes=[pltpu.VMEM((n_heads, n_rows_loc, n_cols), jnp.float32)],
            compiler_params=pltpu.CompilerParams(vmem_limit_bytes=VMEM_LIMIT),
        )(z_tile, gamma, beta, w_b_t)
        bias_t = spread_all(bias_t, "col", n_col_dev).transpose(1, 0, 2, 3).reshape(n_heads, n_query, n_rows_loc)
        bias_t = spread_all(bias_t, "row", mesh.shape["row"]).transpose(1, 2, 0, 3).reshape(n_heads, n_query, n_query)
        z_own = lax.all_to_all(z_tile.reshape(n_col_dev, rows_own, n_cols, pair_dim), "col", 0, 0, tiled=True)
        blk = pl.BlockSpec((n_col_dev, 1, n_cols, pair_dim), lambda i: (0, i, 0, 0))
        u_blk = pl.BlockSpec((n_col_dev, 1, pair_dim, n_cols), lambda i: (0, i, 0, 0))
        u_own = pl.pallas_call(
            attend_kernel,
            grid=(rows_own,),
            in_specs=[blk, whole, whole, whole, whole, whole, whole],
            out_specs=u_blk,
            out_shape=jax.ShapeDtypeStruct((n_col_dev, rows_own, pair_dim, n_cols), jnp.bfloat16),
            scratch_shapes=[
                pltpu.VMEM((n_heads, n_query, n_query), jnp.float32),
                pltpu.VMEM((n_heads, pair_dim, n_query), jnp.bfloat16),
                pltpu.VMEM((pair_dim, n_query), jnp.float32),
            ],
            compiler_params=pltpu.CompilerParams(vmem_limit_bytes=VMEM_LIMIT),
        )(z_own, res_mask.reshape(n_query, 1), bias_t, gamma, beta, w_k, w_qvg_t)
        return lax.all_to_all(u_own, "col", 0, 0, tiled=True).reshape(n_rows_loc, pair_dim, n_cols)

    def local_fn(z_tile, res_mask, ln_gamma, ln_beta, w_q, w_k, w_v, w_g, w_b, w_o):
        n_rows_loc, n_cols, pair_dim = z_tile.shape
        n_heads = w_b.shape[1]
        gamma, beta = ln_gamma[None, :], ln_beta[None, :]
        bf16 = jnp.bfloat16
        w_b_t, w_k_wide, w_qvg_t, eye, logit_bound = pl.pallas_call(
            prepare_kernel,
            in_specs=[whole] * 7,
            out_specs=[whole] * 5,
            out_shape=[
                jax.ShapeDtypeStruct((n_heads, pair_dim), bf16),
                jax.ShapeDtypeStruct((STEP_ROWS * pair_dim, n_heads * pair_dim), bf16),
                jax.ShapeDtypeStruct((3 * pair_dim, pair_dim), bf16),
                jax.ShapeDtypeStruct((n_cols, 2 * n_cols), bf16),
                jax.ShapeDtypeStruct((1, 1), jnp.float32),
            ],
        )(gamma, beta, w_q, w_k, w_v, w_g, w_b)
        u_tile = lax.cond(
            logit_bound[0, 0] < 1e8, functools.partial(fused_path, mesh), whole_keys_path,
            z_tile, res_mask.reshape(-1, n_cols), gamma, beta, w_b_t, w_k, w_k_wide, w_qvg_t, eye)
        rows_step = 64
        z_blk = pl.BlockSpec((rows_step, n_cols, pair_dim), lambda i: (i, 0, 0))
        return pl.pallas_call(
            output_kernel,
            grid=(n_rows_loc // rows_step,),
            in_specs=[z_blk, pl.BlockSpec((rows_step, pair_dim, n_cols), lambda i: (i, 0, 0)), whole],
            out_specs=z_blk,
            out_shape=jax.ShapeDtypeStruct(z_tile.shape, bf16),
            compiler_params=pltpu.CompilerParams(vmem_limit_bytes=VMEM_LIMIT),
        )(z_tile, u_tile, w_o)

    return jax.shard_map(
        local_fn,
        mesh=mesh,
        in_specs=(tile_spec, P("dp"), replicated, replicated, replicated, replicated, replicated, replicated, replicated, replicated),
        out_specs=tile_spec,
        check_vma=False,
    )
```
